32 devices in a mesh: prob: 4 (over y, z), feat: 8 (over x, core).
Axes of the slice: x: 4, y: 2, z: 2, core: 2. Of those that a mesh axis runs over, the one named last changes fastest.
The devices are a block of a 4x4x8 slice.
Arguments:
- design: bfloat16 [65536, 2048], P('prob', 'feat'), parts along dimension 0
- coef_init: float32 [8192, 1], P(('prob', 'feat')), parts along dimension 0
- targets: float32 [65536, 1], P('prob'), parts along dimension 0
- step_sizes: float32 [8192], P(('prob', 'feat')), parts along dimension 0
Outputs:
- output 1: float32 [8192, 1], P(('prob', 'feat')), parts along dimension 0
- output 2: float32 [65536, 1], P('prob'), parts along dimension 0
There are 4 independent parts. The reference program is written for one: setup_inputs(seed, part) draws one part's arguments, and reference() takes and returns one part's arrays. A program takes and returns all parts, laid end to end along the dimension named above; each array names one.
All inputs are finite; a program needn't handle non-finite values.
Results may differ from the reference program's by a relative error of at most 0.00472782.
Values are sent between devices in bfloat16 or wider.
A program may use at most 768 MiB of HBM per device.

```python
import jax
import jax.numpy as jnp
from jax import lax

SAMPLES = 16384
FEAT_DEV = 256
GROUP_SIZE = 8
TARGETS = 1
SWEEPS = 6
FACTORS = 4

FEATURES = FEAT_DEV * GROUP_SIZE
COMBINE_WEIGHT = 0.8
LASSO_WEIGHT = 0.3 * GROUP_SIZE / FEATURES ** 0.5


def setup_inputs(seed: int = 0, part: int = 0) -> dict:
    part_key = jax.random.fold_in(jax.random.key(seed), part)
    draw_keys = jax.random.split(part_key, 9)
    factor_rows = jax.random.normal(draw_keys[0], (SAMPLES, FACTORS), jnp.float32)
    loadings = jax.random.normal(draw_keys[1], (FACTORS, FEATURES), jnp.float32) * (0.5 / FEAT_DEV) ** 0.5

    def draw_block(block_index):
        noise_x = jax.random.normal(jax.random.fold_in(draw_keys[2], block_index), (SAMPLES, FEAT_DEV), jnp.float32)
        load_block = lax.dynamic_slice_in_dim(loadings, block_index * FEAT_DEV, FEAT_DEV, 1)
        x_block = (jnp.dot(factor_rows, load_block) + noise_x).astype(jnp.bfloat16)
        col_sq = jnp.sum(jnp.square(x_block.astype(jnp.float32)), axis=0)
        return x_block, col_sq

    x_blocks, col_sq = lax.map(draw_block, jnp.arange(GROUP_SIZE))
    design = jnp.transpose(x_blocks, (1, 0, 2)).reshape(SAMPLES, FEATURES)
    step_scale = jax.random.uniform(draw_keys[3], (FEATURES,), jnp.float32, 0.5, 1.0)
    step_sizes = step_scale * SAMPLES / (GROUP_SIZE * col_sq.reshape(FEATURES))
    support = jax.random.bernoulli(draw_keys[4], 0.125, (FEATURES, TARGETS)).astype(jnp.float32)
    true_weights = jax.random.normal(draw_keys[5], (FEATURES, TARGETS), jnp.float32) * support * (4.0 / FEATURES) ** 0.5
    factor_weights = jax.random.normal(draw_keys[6], (FACTORS, TARGETS), jnp.float32) * FACTORS ** -0.5
    noise_y = jax.random.normal(draw_keys[7], (SAMPLES, TARGETS), jnp.float32)
    signal = jnp.dot(design, true_weights.astype(jnp.bfloat16), preferred_element_type=jnp.float32)
    targets = jnp.dot(factor_rows, factor_weights) + signal + 0.5 * noise_y
    coef_init = jax.random.normal(draw_keys[8], (FEATURES, TARGETS), jnp.float32) * FEATURES ** -0.5
    return {'design': design, 'coef_init': coef_init, 'targets': targets, 'step_sizes': step_sizes}


def reference(design, coef_init, targets, step_sizes):
    x_blocks = jnp.transpose(design.reshape(SAMPLES, GROUP_SIZE, FEAT_DEV), (1, 0, 2))
    step_col = step_sizes[:, None]
    thresholds = step_col * LASSO_WEIGHT

    def block_sum(values):
        value_blocks = values.astype(jnp.bfloat16).reshape(GROUP_SIZE, FEAT_DEV, TARGETS)

        def add_block(running, operands):
            x_block, v_block = operands
            product = jnp.dot(x_block, v_block, preferred_element_type=jnp.float32).astype(jnp.bfloat16)
            return running + product.astype(jnp.float32), None

        running, _ = lax.scan(add_block, jnp.zeros((SAMPLES, TARGETS), jnp.float32), (x_blocks, value_blocks))
        return running

    residual = targets - block_sum(coef_init)

    def sweep(carry, _):
        weights, residual = carry
        gradient = lax.dot_general(design, residual.astype(jnp.bfloat16), (((0,), (0,)), ((), ())), preferred_element_type=jnp.float32) / SAMPLES
        stepped = weights + step_col * gradient
        shrunk = jnp.sign(stepped) * jnp.maximum(jnp.abs(stepped) - thresholds, 0.0)
        change = shrunk - weights
        weights = weights + COMBINE_WEIGHT * change
        residual = residual - COMBINE_WEIGHT * block_sum(change)
        return (weights, residual), None

    (weights, residual), _ = lax.scan(sweep, (coef_init, residual), None, length=SWEEPS)
    return (weights, residual)
```

```python
import functools

import jax
import jax.numpy as jnp
from jax import lax
from jax.experimental import pallas as pl
from jax.experimental.pallas import tpu as pltpu
from jax.sharding import PartitionSpec as P

SWEEPS = 6
COMBINE_WEIGHT = 0.8
MESH = pl.DeviceIdType.MESH
LANES = 128
ROWS = 16
CHUNK = 2 * ROWS * LANES
LOADS = 8


def kernel(size, lasso_weight, x_hbm, w_ref, y_ref, eta_ref, w_out, r_out, xv, xt, ubuf, rbf, res, dmat, wcur, load_sem, send_sem, recv_sem, rsend_sem, rrecv_sem):
    samples, feats = x_hbm.shape
    chunks = samples // CHUNK
    qrows = CHUNK // LANES
    chips = size // 2
    me = lax.axis_index('feat')
    chip, core = me // 2, lax.rem(me, 2)
    sibling = 2 * chip + 1 - core
    lead = core == 1

    load_rows = samples // LOADS
    loads = [pltpu.make_async_copy(x_hbm.at[pl.ds(i * load_rows, load_rows)], xv.at[pl.ds(i * load_rows, load_rows)], load_sem.at[i]) for i in range(LOADS)]
    for load in loads:
        load.start()

    barrier = pltpu.get_barrier_semaphore()
    for d in range(1, size):
        pl.semaphore_signal(barrier, inc=1, device_id={'feat': lax.rem(me + d, size)}, device_id_type=MESH)

    row_id = lax.broadcasted_iota(jnp.int32, (ROWS, LANES), 0)

    def set_dmat(values):
        for h in range(feats // LANES):
            piece = jnp.broadcast_to(values[:, h * LANES:(h + 1) * LANES], (ROWS, LANES))
            for m in range(ROWS):
                dmat[:, m * feats + h * LANES:m * feats + (h + 1) * LANES] = jnp.where(row_id == m, piece, 0.0).astype(jnp.bfloat16)

    def u_copy(par, g, dest, slot):
        here = ubuf.at[par, me, pl.ds(g * qrows, qrows)]
        return pltpu.make_async_remote_copy(src_ref=here, dst_ref=here, send_sem=send_sem.at[g, slot], recv_sem=recv_sem.at[par, g, me], device_id={'feat': dest}, device_id_type=MESH)

    far_order = [chips // 2] + [d for d in range(1, chips) if d != chips // 2]

    def u_chunk(par, g):
        u = jnp.dot(dmat[...], xt[pl.ds(g * CHUNK, CHUNK), :], preferred_element_type=jnp.float32).astype(jnp.bfloat16)
        ubuf[par, me, pl.ds(g * qrows, ROWS), :] = u[:, :LANES]
        ubuf[par, me, pl.ds(g * qrows + ROWS, ROWS), :] = u[:, LANES:]
        for slot, d in enumerate(far_order):
            u_copy(par, g, 2 * lax.rem(chip + d, chips) + 1, slot).start()

        @pl.when(core == 0)
        def _():
            u_copy(par, g, sibling, chips - 1).start()

    def u_wait_sends(par):
        for g in range(chunks):
            for slot in range(chips - 1):
                u_copy(par, g, sibling, slot).wait_send()

            @pl.when(core == 0)
            def _():
                u_copy(par, g, sibling, chips - 1).wait_send()

    def r_copy(buf, g):
        here = buf.at[pl.ds(g * qrows, qrows)]
        return pltpu.make_async_remote_copy(src_ref=here, dst_ref=here, send_sem=rsend_sem.at[g], recv_sem=rrecv_sem.at[g], device_id={'feat': sibling}, device_id_type=MESH)

    def new_residual(par, g, factor):
        for d in range(1, size):
            src = lax.rem(me + d, size)
            there = ubuf.at[par, src, pl.ds(g * qrows, qrows)]
            pltpu.make_async_remote_copy(src_ref=there, dst_ref=there, send_sem=send_sem.at[g, 0], recv_sem=recv_sem.at[par, g, src], device_id={'feat': src}, device_id_type=MESH).wait_recv()
        total = ubuf[par, 0, pl.ds(g * qrows, qrows), :].astype(jnp.float32)
        for s in range(1, size):
            total = total + ubuf[par, s, pl.ds(g * qrows, qrows), :].astype(jnp.float32)
        return res[pl.ds(g * qrows, qrows), :] - factor * total

    res[...] = y_ref[...]
    wcur[...] = w_ref[...]
    set_dmat(w_ref[...])

    per_chunk = LOADS // chunks
    for g in range(chunks):
        for i in range(per_chunk):
            loads[g * per_chunk + i].wait()

        @pl.loop(0, ROWS)
        def _(m):
            for h in range(2):
                src = pl.multiple_of(g * CHUNK + h * ROWS * LANES + m * LANES, LANES)
                dst = pl.multiple_of(g * CHUNK + m * feats, feats)
                xt[pl.ds(dst, feats), h * LANES:(h + 1) * LANES] = xv[pl.ds(src, LANES), :].T

    pl.semaphore_wait(barrier, size - 1)

    @pl.loop(0, SWEEPS)
    def _(t):
        par = lax.rem(t, 2)
        factor = jnp.where(t == 0, 1.0, COMBINE_WEIGHT).astype(jnp.float32)
        for g in range(chunks):
            u_chunk(par, g)

        grad = jnp.zeros((ROWS, feats), jnp.float32)
        for g in range(chunks):
            @pl.when(lead)
            def _():
                r = new_residual(par, g, factor)
                res[pl.ds(g * qrows, qrows), :] = r
                rbf[pl.ds(g * qrows, qrows), :] = r.astype(jnp.bfloat16)
                r_copy(rbf, g).start()

            @pl.when(core == 0)
            def _():
                r_copy(rbf, g).wait_recv()

            zero = jnp.zeros((ROWS, LANES), jnp.float32)
            halves = [rbf[pl.ds(g * qrows + h * ROWS, ROWS), :].astype(jnp.float32) for h in range(2)]
            left = jnp.concatenate([jnp.where(row_id == m, halves[h], zero).astype(jnp.bfloat16) for h in range(2) for m in range(ROWS)], axis=1)
            grad = grad + jnp.dot(left, xv[pl.ds(g * CHUNK, CHUNK), :], preferred_element_type=jnp.float32)

        gradient = jnp.sum(grad, axis=0, keepdims=True) * (1.0 / samples)
        weights = wcur[...]
        eta = eta_ref[...]
        threshold = eta * lasso_weight
        stepped = weights + eta * gradient
        shrunk = jnp.maximum(stepped - threshold, 0.0) + jnp.minimum(stepped + threshold, 0.0)
        change = shrunk - weights
        wcur[...] = weights + COMBINE_WEIGHT * change
        set_dmat(change)
        u_wait_sends(par)

        @pl.when(lead)
        def _():
            for g in range(chunks):
                r_copy(rbf, g).wait_send()

    last = SWEEPS % 2
    for g in range(chunks):
        u_chunk(last, g)
    w_out[...] = wcur[...]
    for g in range(chunks):
        @pl.when(lead)
        def _():
            res[pl.ds(g * qrows, qrows), :] = new_residual(last, g, COMBINE_WEIGHT)
            r_copy(res, g).start()
    for g in range(chunks):
        @pl.when(core == 0)
        def _():
            r_copy(res, g).wait_recv()
    r_out[...] = res[...]
    u_wait_sends(last)

    @pl.when(lead)
    def _():
        for g in range(chunks):
            r_copy(res, g).wait_send()


def solution(mesh):
    size = mesh.shape['feat']

    def local_run(x_local, coef_local, targets_local, step_local):
        samples, feats = x_local.shape
        chunks = samples // CHUNK
        lasso_weight = 0.3 * size / (feats * size) ** 0.5
        vmem = pl.BlockSpec(memory_space=pltpu.VMEM)
        weights, residual = pl.pallas_call(
            functools.partial(kernel, size, lasso_weight),
            out_shape=(jax.ShapeDtypeStruct((1, feats), jnp.float32), jax.ShapeDtypeStruct((samples // LANES, LANES), jnp.float32)),
            in_specs=[pl.BlockSpec(memory_space=pl.ANY), vmem, vmem, vmem],
            out_specs=(vmem, vmem),
            scratch_shapes=[
                pltpu.VMEM((samples, feats), jnp.bfloat16),
                pltpu.VMEM((samples, feats), jnp.bfloat16),
                pltpu.VMEM((2, size, samples // LANES, LANES), jnp.bfloat16),
                pltpu.VMEM((samples // LANES, LANES), jnp.bfloat16),
                pltpu.VMEM((samples // LANES, LANES), jnp.float32),
                pltpu.VMEM((ROWS, ROWS * feats), jnp.bfloat16),
                pltpu.VMEM((1, feats), jnp.float32),
                pltpu.SemaphoreType.DMA((LOADS,)),
                pltpu.SemaphoreType.DMA((chunks, size // 2)),
                pltpu.SemaphoreType.DMA((2, chunks, size)),
                pltpu.SemaphoreType.DMA((chunks,)),
                pltpu.SemaphoreType.DMA((chunks,)),
            ],
            compiler_params=pltpu.CompilerParams(collective_id=0, has_side_effects=True),
        )(x_local, coef_local.reshape(1, feats), targets_local.reshape(samples // LANES, LANES), step_local.reshape(1, feats))
        return weights.reshape(feats, 1), residual.reshape(samples, 1)

    return jax.shard_map(local_run, mesh=mesh, in_specs=(P('prob', 'feat'), P(('prob', 'feat'), None), P('prob', None), P(('prob', 'feat'))), out_specs=(P(('prob', 'feat'), None), P('prob', None)), check_vma=False)
```

```python
import functools

import jax
import jax.numpy as jnp
from jax import lax
from jax.experimental import pallas as pl
from jax.experimental.pallas import tpu as pltpu
from jax.sharding import PartitionSpec as P

SWEEPS = 6
COMBINE_WEIGHT = 0.8
MESH = pl.DeviceIdType.MESH
LANES = 128
SUB = 8
TILE = 2 * LANES
UNIT = SUB * TILE
CHUNK = 2 * UNIT


def kernel(size, lasso_weight, x_hbm, w_ref, y_ref, eta_ref, w_out, r_out, xv, xt, ubuf, rbf, res, dmat, wcur, load_sem, send_sem, recv_sem, rsend_sem, rrecv_sem):
    samples = x_hbm.shape[0]
    chunks = samples // CHUNK
    qrows = CHUNK // LANES
    chips = size // 2
    me = lax.axis_index('feat')
    chip, core = me // 2, lax.rem(me, 2)
    sibling = 2 * chip + 1 - core
    lead = core == 1
    far_order = [chips // 2] + [d for d in range(1, chips) if d != chips // 2]

    loads = [pltpu.make_async_copy(x_hbm.at[pl.ds(g * CHUNK, CHUNK)], xv.at[pl.ds(g * CHUNK, CHUNK)], load_sem.at[g]) for g in range(chunks)]
    for load in loads:
        load.start()

    barrier = pltpu.get_barrier_semaphore()
    for d in range(1, size):
        pl.semaphore_signal(barrier, inc=1, device_id={'feat': lax.rem(me + d, size)}, device_id_type=MESH)

    row_id = lax.broadcasted_iota(jnp.int32, (SUB, TILE), 0)

    def set_dmat(values):
        spread = jnp.broadcast_to(values, (SUB, TILE))
        for m in range(SUB):
            dmat[:, m * TILE:(m + 1) * TILE] = jnp.where(row_id == m, spread, 0.0).astype(jnp.bfloat16)

    def u_copy(par, g, dest, slot):
        here = ubuf.at[par, me, pl.ds(g * qrows, qrows)]
        return pltpu.make_async_remote_copy(src_ref=here, dst_ref=here, send_sem=send_sem.at[par, g, slot], recv_sem=recv_sem.at[par, g, me], device_id={'feat': dest}, device_id_type=MESH)

    def u_half(g, part):
        out = []
        for q in range(2):
            base = (2 * g + q) * UNIT + part * UNIT // 2
            left = dmat[:, part * UNIT // 2:(part + 1) * UNIT // 2]
            out.append(jnp.dot(left, xt[pl.ds(base, UNIT // 2), :], preferred_element_type=jnp.float32))
        return out

    def u_first(g, part):
        out = []
        for q in range(2):
            base = (2 * g + q) * UNIT
            left = dmat[:, part * UNIT // 2:(part + 1) * UNIT // 2]
            rhs = jnp.concatenate([jnp.concatenate([xv[pl.ds(base + (h * SUB + m) * LANES, LANES), :] for h in range(2)], axis=0) for m in range(part * SUB // 2, (part + 1) * SUB // 2)], axis=1)
            out.append(lax.dot_general(left, rhs, (((1,), (1,)), ((), ())), preferred_element_type=jnp.float32))
        return out

    def u_finish(par, g, halves):
        for q in range(2):
            u = halves[0][q] + halves[1][q]
            u = jnp.concatenate([u[:, :LANES], u[:, LANES:]], axis=0).astype(jnp.bfloat16)
            ubuf[par, me, pl.ds(g * qrows + q * 2 * SUB, 2 * SUB), :] = u
        for slot, d in enumerate(far_order):
            u_copy(par, g, 2 * lax.rem(chip + d, chips) + 1, slot).start()

        @pl.when(core == 0)
        def _():
            u_copy(par, g, sibling, chips - 1).start()

    def products(par):
        start = u_half(0, 0)
        for g in range(chunks):
            end = u_half(g, 1)
            following = u_half(g + 1, 0) if g + 1 < chunks else None
            u_finish(par, g, (start, end))
            start = following

    def u_wait_sends(par):
        for g in range(chunks):
            for slot in range(chips - 1):
                u_copy(par, g, sibling, slot).wait_send()

            @pl.when(core == 0)
            def _():
                u_copy(par, g, sibling, chips - 1).wait_send()

    def r_copy(buf, g):
        here = buf.at[pl.ds(g * qrows, qrows)]
        return pltpu.make_async_remote_copy(src_ref=here, dst_ref=here, send_sem=rsend_sem.at[g], recv_sem=rrecv_sem.at[g], device_id={'feat': sibling}, device_id_type=MESH)

    def new_residual(par, g, factor):
        for d in range(1, size):
            src = lax.rem(me + d, size)
            there = ubuf.at[par, src, pl.ds(g * qrows, qrows)]
            pltpu.make_async_remote_copy(src_ref=there, dst_ref=there, send_sem=send_sem.at[par, g, 0], recv_sem=recv_sem.at[par, g, src], device_id={'feat': src}, device_id_type=MESH).wait_recv()
        total = ubuf[par, 0, pl.ds(g * qrows, qrows), :].astype(jnp.float32)
        for s in range(1, size):
            total = total + ubuf[par, s, pl.ds(g * qrows, qrows), :].astype(jnp.float32)
        return res[pl.ds(g * qrows, qrows), :] - factor * total

    def residual_and_gradient(par, factor):
        grads = [jnp.zeros((SUB, TILE), jnp.float32)] * 2
        for g in range(chunks):
            @pl.when(lead)
            def _():
                r = new_residual(par, g, factor)
                res[pl.ds(g * qrows, qrows), :] = r
                rbf[pl.ds(g * qrows, qrows), :] = r.astype(jnp.bfloat16)
                r_copy(rbf, g).start()

            @pl.when(core == 0)
            def _():
                r_copy(rbf, g).wait_recv()

            r = rbf[pl.ds(g * qrows, qrows), :].astype(jnp.float32)
            for q in range(2):
                pieces = []
                for k in range(2 * SUB):
                    base = q * 2 * SUB + k // SUB * SUB
                    pieces.append(jnp.where(row_id[:, :LANES] == k % SUB, r[base:base + SUB], 0.0).astype(jnp.bfloat16))
                left = jnp.concatenate(pieces, axis=1)
                grads[q] = grads[q] + jnp.dot(left, xv[pl.ds((2 * g + q) * UNIT, UNIT), :], preferred_element_type=jnp.float32)
        total = jnp.sum(grads[0], axis=0, keepdims=True) + jnp.sum(grads[1], axis=0, keepdims=True)
        return total * (1.0 / samples)

    def update(gradient):
        weights = wcur[...]
        eta = eta_ref[...]
        threshold = eta * lasso_weight
        stepped = weights + eta * gradient
        shrunk = jnp.maximum(stepped - threshold, 0.0) + jnp.minimum(stepped + threshold, 0.0)
        change = shrunk - weights
        wcur[...] = weights + COMBINE_WEIGHT * change
        set_dmat(change)

    def sweep_end(par):
        u_wait_sends(par)

        @pl.when(lead)
        def _():
            for g in range(chunks):
                r_copy(rbf, g).wait_send()

    res[...] = y_ref[...]
    wcur[...] = w_ref[...]
    set_dmat(w_ref[...])

    for g in range(chunks):
        loads[g].wait()
        halves = [u_first(g, part) for part in range(2)]
        if g == 0:
            pl.semaphore_wait(barrier, size - 1)
        u_finish(0, g, halves)

    @pl.loop(0, samples // UNIT)
    def _(unit):
        for m in range(SUB):
            for h in range(2):
                src = pl.multiple_of(unit * UNIT + h * SUB * LANES + m * LANES, LANES)
                dst = pl.multiple_of(unit * UNIT + m * TILE, TILE)
                xt[pl.ds(dst, TILE), h * LANES:(h + 1) * LANES] = xv[pl.ds(src, LANES), :].T

    @pl.loop(0, SWEEPS)
    def _(t):
        par = lax.rem(t, 2)
        factor = jnp.where(t == 0, 1.0, COMBINE_WEIGHT).astype(jnp.float32)
        update(residual_and_gradient(par, factor))
        products(1 - par)
        sweep_end(par)

    last = SWEEPS % 2
    w_out[...] = wcur[...]
    for g in range(chunks):
        @pl.when(lead)
        def _():
            res[pl.ds(g * qrows, qrows), :] = new_residual(last, g, COMBINE_WEIGHT)
            r_copy(res, g).start()
    for g in range(chunks):
        @pl.when(core == 0)
        def _():
            r_copy(res, g).wait_recv()
    r_out[...] = res[...]
    u_wait_sends(last)

    @pl.when(lead)
    def _():
        for g in range(chunks):
            r_copy(res, g).wait_send()


def solution(mesh):
    size = mesh.shape['feat']

    def local_run(x_local, coef_local, targets_local, step_local):
        samples, feats = x_local.shape
        chunks = samples // CHUNK
        lasso_weight = 0.3 * size / (feats * size) ** 0.5
        vmem = pl.BlockSpec(memory_space=pltpu.VMEM)
        weights, residual = pl.pallas_call(
            functools.partial(kernel, size, lasso_weight),
            out_shape=(jax.ShapeDtypeStruct((1, feats), jnp.float32), jax.ShapeDtypeStruct((samples // LANES, LANES), jnp.float32)),
            in_specs=[pl.BlockSpec(memory_space=pl.ANY), vmem, vmem, vmem],
            out_specs=(vmem, vmem),
            scratch_shapes=[
                pltpu.VMEM((samples, feats), jnp.bfloat16),
                pltpu.VMEM((samples, feats), jnp.bfloat16),
                pltpu.VMEM((2, size, samples // LANES, LANES), jnp.bfloat16),
                pltpu.VMEM((samples // LANES, LANES), jnp.bfloat16),
                pltpu.VMEM((samples // LANES, LANES), jnp.float32),
                pltpu.VMEM((SUB, SUB * feats), jnp.bfloat16),
                pltpu.VMEM((1, feats), jnp.float32),
                pltpu.SemaphoreType.DMA((chunks,)),
                pltpu.SemaphoreType.DMA((2, chunks, size // 2)),
                pltpu.SemaphoreType.DMA((2, chunks, size)),
                pltpu.SemaphoreType.DMA((chunks,)),
                pltpu.SemaphoreType.DMA((chunks,)),
            ],
            compiler_params=pltpu.CompilerParams(collective_id=0, has_side_effects=True),
        )(x_local, coef_local.reshape(1, feats), targets_local.reshape(samples // LANES, LANES), step_local.reshape(1, feats))
        return weights.reshape(feats, 1), residual.reshape(samples, 1)

    return jax.shard_map(local_run, mesh=mesh, in_specs=(P('prob', 'feat'), P(('prob', 'feat'), None), P('prob', None), P(('prob', 'feat'))), out_specs=(P(('prob', 'feat'), None), P('prob', None)), check_vma=False)
```

```python
import functools

import jax
import jax.numpy as jnp
from jax import lax
from jax.experimental import pallas as pl
from jax.experimental.pallas import tpu as pltpu
from jax.sharding import PartitionSpec as P

SWEEPS = 6
COMBINE_WEIGHT = 0.8
MESH = pl.DeviceIdType.MESH
LANES = 128
SUB = 8
ROWS = 16
TILE = 2 * LANES
BLOCK = ROWS * TILE
QROWS = BLOCK // LANES
MATMUL_ROWS = 10
SECTIONS = ((0, 2), (2, 4))


def kernel(size, lasso_weight, x_hbm, w_hbm, y_hbm, eta_hbm, w_out, r_out, xv, xt, ubuf, rbf, res, dmat, dcol, gref, wcur, eta_v, load_sem, small_sem, send_sem, recv_sem, rsend_sem, rrecv_sem):
    samples = x_hbm.shape[0]
    blocks = samples // BLOCK
    chips = size // 2
    me = lax.axis_index('feat')
    chip, core = me // 2, lax.rem(me, 2)
    sibling = 2 * chip + 1 - core
    lead = core == 1
    far_order = [chips // 2] + [d for d in range(1, chips) if d != chips // 2]

    small = [pltpu.make_async_copy(src, dst, small_sem.at[i]) for i, (src, dst) in enumerate(((w_hbm, wcur), (eta_hbm, eta_v), (y_hbm, res)))]
    loads = [pltpu.make_async_copy(x_hbm.at[pl.ds(b * BLOCK, BLOCK)], xv.at[pl.ds(b * BLOCK, BLOCK)], load_sem.at[b]) for b in range(blocks)]
    small[0].start()
    for load in loads:
        load.start()
    for load in small[1:]:
        load.start()

    barrier = pltpu.get_barrier_semaphore()
    for d in range(1, size):
        pl.semaphore_signal(barrier, inc=1, device_id={'feat': lax.rem(me + d, size)}, device_id_type=MESH)

    row16 = lax.broadcasted_iota(jnp.int32, (ROWS, LANES), 0)
    row8 = lax.broadcasted_iota(jnp.int32, (SUB, LANES), 0)

    def set_left(values, rows):
        for h in range(2):
            spread = jnp.broadcast_to(values[:, h * LANES:(h + 1) * LANES], (ROWS, LANES))
            for m in range(rows):
                dmat[:, m * TILE + h * LANES:m * TILE + (h + 1) * LANES] = jnp.where(row16 == m, spread, 0.0).astype(jnp.bfloat16)

    def set_column(values):
        rounded = values.astype(jnp.bfloat16).astype(jnp.float32)
        for h in range(2):
            dcol[h * LANES:(h + 1) * LANES, :] = jnp.broadcast_to(rounded[:, h * LANES:(h + 1) * LANES], (LANES, LANES)).T

    def rows_of(s):
        first, last = SECTIONS[s]
        return pl.ds(first * QROWS, (last - first) * QROWS)

    def u_copy(par, s, dest, slot):
        here = ubuf.at[par, me, rows_of(s)]
        return pltpu.make_async_remote_copy(src_ref=here, dst_ref=here, send_sem=send_sem.at[par, s, slot], recv_sem=recv_sem.at[par, s, me], device_id={'feat': dest}, device_id_type=MESH)

    def u_send(par, s):
        for slot, d in enumerate(far_order):
            u_copy(par, s, 2 * lax.rem(chip + d, chips) + 1, slot).start()

        @pl.when(core == 0)
        def _():
            u_copy(par, s, sibling, chips - 1).start()

    def u_wait_sends(par):
        for s in range(len(SECTIONS)):
            for slot in range(chips - 1):
                u_copy(par, s, sibling, slot).wait_send()

            @pl.when(core == 0)
            def _():
                u_copy(par, s, sibling, chips - 1).wait_send()

    def u_store(par, b, h, values):
        ubuf[par, me, pl.ds(b * QROWS + h * ROWS, ROWS), :] = values.astype(jnp.bfloat16)

    def first_products(b):
        rhs = []
        for m in range(ROWS):
            rhs.append(jnp.concatenate([xv[pl.ds(b * BLOCK + (h * ROWS + m) * LANES, LANES), :] for h in range(2)], axis=0))
        half = ROWS // 2
        out = []
        for p in range(2):
            left = dmat[:, p * half * TILE:(p + 1) * half * TILE]
            right = jnp.concatenate(rhs[p * half:(p + 1) * half], axis=1)
            out.append(lax.dot_general(left, right, (((1,), (1,)), ((), ())), preferred_element_type=jnp.float32))
        for h in range(2):
            cols = slice(h * LANES, (h + 1) * LANES)
            u_store(0, b, h, jnp.where(row16 < half, out[0][:, cols], out[1][:, cols]))

    def transpose_block(b):
        for m in range(ROWS):
            for h in range(2):
                xt[pl.ds(b * BLOCK + m * TILE, TILE), h * LANES:(h + 1) * LANES] = xv[pl.ds(b * BLOCK + (h * ROWS + m) * LANES, LANES), :].T

    def vector_products(b, h):
        accs = [None] * (ROWS - MATMUL_ROWS)
        for f in range(0, TILE, ROWS):
            d = dcol[f:f + ROWS, :]
            for i in range(len(accs)):
                t = xt[pl.ds(b * BLOCK + (MATMUL_ROWS + i) * TILE + f, ROWS), h * LANES:(h + 1) * LANES].astype(jnp.float32) * d
                t = t[:SUB] + t[SUB:]
                accs[i] = t if accs[i] is None else accs[i] + t
        return [jnp.sum(a, axis=0, keepdims=True) for a in accs]

    def section_products(par, s):
        first, last = SECTIONS[s]
        for b in range(first, last):
            if last - first > 1:
                u = jnp.dot(dmat[:, :MATMUL_ROWS * TILE], xt[pl.ds(b * BLOCK, MATMUL_ROWS * TILE), :], preferred_element_type=jnp.float32)
                parts = [u[:, :LANES], u[:, LANES:]]
            else:
                half = MATMUL_ROWS // 2
                out = [jnp.dot(dmat[:, p * half * TILE:(p + 1) * half * TILE], xt[pl.ds(b * BLOCK + p * half * TILE, half * TILE), :], preferred_element_type=jnp.float32) for p in range(2)]
                parts = [jnp.where(row16 < half, out[0][:, cols], out[1][:, cols]) for cols in (slice(0, LANES), slice(LANES, TILE))]
            for h in range(2):
                high = parts[h][SUB:]
                for i, total in enumerate(vector_products(b, h)):
                    high = jnp.where(row8 == MATMUL_ROWS + i - SUB, total, high)
                u_store(par, b, h, jnp.concatenate([parts[h][:SUB], high], axis=0))

    def products(par):
        for s in range(len(SECTIONS)):
            section_products(par, s)
            u_send(par, s)

    def r_copy(buf, s):
        here = buf.at[rows_of(s)]
        return pltpu.make_async_remote_copy(src_ref=here, dst_ref=here, send_sem=rsend_sem.at[s], recv_sem=rrecv_sem.at[s], device_id={'feat': sibling}, device_id_type=MESH)

    def new_residual(par, s, factor):
        rows = rows_of(s)
        for d in range(1, size):
            src = lax.rem(me + d, size)
            there = ubuf.at[par, src, rows]
            pltpu.make_async_remote_copy(src_ref=there, dst_ref=there, send_sem=send_sem.at[par, s, 0], recv_sem=recv_sem.at[par, s, src], device_id={'feat': src}, device_id_type=MESH).wait_recv()
        total = ubuf[par, 0, rows, :].astype(jnp.float32)
        for k in range(1, size):
            total = total + ubuf[par, k, rows, :].astype(jnp.float32)
        return res[rows, :] - factor * total

    def gradient(par, factor):
        for s in range(len(SECTIONS)):
            first, last = SECTIONS[s]
            rows = rows_of(s)

            @pl.when(lead)
            def _():
                r = new_residual(par, s, factor)
                res[rows, :] = r
                rbf[rows, :] = r.astype(jnp.bfloat16)
                r_copy(rbf, s).start()

            @pl.when(core == 0)
            def _():
                r_copy(rbf, s).wait_recv()

            pieces = []
            for k in range(first * QROWS, last * QROWS):
                r16 = rbf[pl.ds(k // ROWS * ROWS, ROWS), :]
                pieces.append(jnp.where(row16 == k % ROWS, r16.astype(jnp.float32), 0.0).astype(jnp.bfloat16))
            half = len(pieces) // 2
            sums = []
            for q in range(2):
                left = jnp.concatenate(pieces[q * half:(q + 1) * half], axis=1)
                g = jnp.dot(left, xv[pl.ds(first * BLOCK + q * half * LANES, half * LANES), :], preferred_element_type=jnp.float32)
                if s:
                    g = gref[q] + g
                if s < len(SECTIONS) - 1:
                    gref[q] = g
                sums.append(jnp.sum(g, axis=0, keepdims=True))
        return (sums[0] + sums[1]) * (1.0 / samples)

    def update(grad):
        weights = wcur[...]
        eta = eta_v[...]
        threshold = eta * lasso_weight
        stepped = weights + eta * grad
        shrunk = jnp.maximum(stepped - threshold, 0.0) + jnp.minimum(stepped + threshold, 0.0)
        change = shrunk - weights
        wcur[...] = weights + COMBINE_WEIGHT * change
        set_left(change, MATMUL_ROWS)
        set_column(change)

    small[0].wait()
    set_left(wcur[...], ROWS)
    for s, (first, last) in enumerate(SECTIONS):
        for b in range(first, last):
            loads[b].wait()
            first_products(b)
            transpose_block(b)
        if s == 0:
            pl.semaphore_wait(barrier, size - 1)
        u_send(0, s)
    small[1].wait()
    small[2].wait()

    @pl.loop(0, SWEEPS)
    def _(t):
        par = lax.rem(t, 2)
        factor = jnp.where(t == 0, 1.0, COMBINE_WEIGHT).astype(jnp.float32)
        update(gradient(par, factor))
        products(1 - par)
        u_wait_sends(par)

        @pl.when(lead)
        def _():
            for s in range(len(SECTIONS)):
                r_copy(rbf, s).wait_send()

    par = SWEEPS % 2
    w_out[...] = wcur[...]
    for s in range(len(SECTIONS)):
        @pl.when(lead)
        def _():
            res[rows_of(s), :] = new_residual(par, s, COMBINE_WEIGHT)
            r_copy(res, s).start()
    for s in range(len(SECTIONS)):
        @pl.when(core == 0)
        def _():
            r_copy(res, s).wait_recv()
    r_out[...] = res[...]
    u_wait_sends(par)

    @pl.when(lead)
    def _():
        for s in range(len(SECTIONS)):
            r_copy(res, s).wait_send()


def solution(mesh):
    size = mesh.shape['feat']

    def local_run(x_local, coef_local, targets_local, step_local):
        samples, feats = x_local.shape
        sections = len(SECTIONS)
        lasso_weight = 0.3 * size / (feats * size) ** 0.5
        vmem = pl.BlockSpec(memory_space=pltpu.VMEM)
        anywhere = pl.BlockSpec(memory_space=pl.ANY)
        weights, residual = pl.pallas_call(
            functools.partial(kernel, size, lasso_weight),
            out_shape=(jax.ShapeDtypeStruct((1, feats), jnp.float32), jax.ShapeDtypeStruct((samples // LANES, LANES), jnp.float32)),
            in_specs=[anywhere] * 4,
            out_specs=(vmem, vmem),
            scratch_shapes=[
                pltpu.VMEM((samples, feats), jnp.bfloat16),
                pltpu.VMEM((samples, feats), jnp.bfloat16),
                pltpu.VMEM((2, size, samples // LANES, LANES), jnp.bfloat16),
                pltpu.VMEM((samples // LANES, LANES), jnp.bfloat16),
                pltpu.VMEM((samples // LANES, LANES), jnp.float32),
                pltpu.VMEM((ROWS, ROWS * feats), jnp.bfloat16),
                pltpu.VMEM((feats, LANES), jnp.float32),
                pltpu.VMEM((2, ROWS, feats), jnp.float32),
                pltpu.VMEM((1, feats), jnp.float32),
                pltpu.VMEM((1, feats), jnp.float32),
                pltpu.SemaphoreType.DMA((samples // BLOCK,)),
                pltpu.SemaphoreType.DMA((3,)),
                pltpu.SemaphoreType.DMA((2, sections, size // 2)),
                pltpu.SemaphoreType.DMA((2, sections, size)),
                pltpu.SemaphoreType.DMA((sections,)),
                pltpu.SemaphoreType.DMA((sections,)),
            ],
            compiler_params=pltpu.CompilerParams(collective_id=0, has_side_effects=True),
        )(x_local, coef_local.reshape(1, feats), targets_local.reshape(samples // LANES, LANES), step_local.reshape(1, feats))
        return weights.reshape(feats, 1), residual.reshape(samples, 1)

    return jax.shard_map(local_run, mesh=mesh, in_specs=(P('prob', 'feat'), P(('prob', 'feat'), None), P('prob', None), P(('prob', 'feat'))), out_specs=(P(('prob', 'feat'), None), P('prob', None)), check_vma=False)
```

```python
import functools

import jax
import jax.numpy as jnp
from jax import lax
from jax.experimental import pallas as pl
from jax.experimental.pallas import tpu as pltpu
from jax.sharding import PartitionSpec as P

SWEEPS = 6
COMBINE_WEIGHT = 0.8
MESH = pl.DeviceIdType.MESH
LANES = 128
SUB = 8
ROWS = 16
TILE = 2 * LANES
BLOCK = ROWS * TILE
QROWS = BLOCK // LANES
MATMUL_ROWS = 10
FENCE = 4
SECTIONS = ((0, 2), (2, 4))


def kernel(size, lasso_weight, x_hbm, w_hbm, y_hbm, eta_hbm, w_out, r_out, xv, xt, ubuf, rbf, res, dmat, dcol, gref, wcur, eta_v, load_sem, small_sem, send_sem, recv_sem, rsend_sem, rrecv_sem):
    samples = x_hbm.shape[0]
    blocks = samples // BLOCK
    chips = size // 2
    me = lax.axis_index('feat')
    chip, core = me // 2, lax.rem(me, 2)
    sibling = 2 * chip + 1 - core
    lead = core == 1
    far_order = [chips // 2] + [d for d in range(1, chips) if d != chips // 2]

    small = [pltpu.make_async_copy(src, dst, small_sem.at[i]) for i, (src, dst) in enumerate(((w_hbm, wcur), (eta_hbm, eta_v), (y_hbm, res)))]
    loads = [pltpu.make_async_copy(x_hbm.at[pl.ds(b * BLOCK, BLOCK)], xv.at[pl.ds(b * BLOCK, BLOCK)], load_sem.at[b]) for b in range(blocks)]
    small[0].start()
    for load in loads:
        load.start()
    for load in small[1:]:
        load.start()

    barrier = pltpu.get_barrier_semaphore()
    for d in range(1, size):
        pl.semaphore_signal(barrier, inc=1, device_id={'feat': lax.rem(me + d, size)}, device_id_type=MESH)

    row16 = lax.broadcasted_iota(jnp.int32, (ROWS, LANES), 0)
    row8 = lax.broadcasted_iota(jnp.int32, (SUB, LANES), 0)

    def set_left(values, rows):
        for h in range(2):
            spread = jnp.broadcast_to(values[:, h * LANES:(h + 1) * LANES], (ROWS, LANES))
            for m in range(rows):
                dmat[:, m * TILE + h * LANES:m * TILE + (h + 1) * LANES] = jnp.where(row16 == m, spread, 0.0).astype(jnp.bfloat16)

    def set_column(values):
        rounded = values.astype(jnp.bfloat16).astype(jnp.float32)
        for h in range(2):
            dcol[h * LANES:(h + 1) * LANES, :] = jnp.broadcast_to(rounded[:, h * LANES:(h + 1) * LANES], (LANES, LANES)).T

    def rows_of(s):
        first, last = SECTIONS[s]
        return pl.ds(first * QROWS, (last - first) * QROWS)

    def u_copy(par, s, dest, slot):
        here = ubuf.at[par, me, rows_of(s)]
        return pltpu.make_async_remote_copy(src_ref=here, dst_ref=here, send_sem=send_sem.at[par, s, slot], recv_sem=recv_sem.at[par, s, me], device_id={'feat': dest}, device_id_type=MESH)

    def u_send(par, s):
        for slot, d in enumerate(far_order):
            u_copy(par, s, 2 * lax.rem(chip + d, chips) + 1, slot).start()

        @pl.when(core == 0)
        def _():
            u_copy(par, s, sibling, chips - 1).start()

    def u_wait_sends(par):
        for s in range(len(SECTIONS)):
            for slot in range(chips - 1):
                u_copy(par, s, sibling, slot).wait_send()

            @pl.when(core == 0)
            def _():
                u_copy(par, s, sibling, chips - 1).wait_send()

    def u_store(par, b, h, values):
        ubuf[par, me, pl.ds(b * QROWS + h * ROWS, ROWS), :] = values.astype(jnp.bfloat16)

    def first_products(b):
        rhs = []
        for m in range(ROWS):
            rhs.append(jnp.concatenate([xv[pl.ds(b * BLOCK + (h * ROWS + m) * LANES, LANES), :] for h in range(2)], axis=0))
        half = ROWS // 2
        out = []
        for p in range(2):
            left = dmat[:, p * half * TILE:(p + 1) * half * TILE]
            right = jnp.concatenate(rhs[p * half:(p + 1) * half], axis=1)
            out.append(lax.dot_general(left, right, (((1,), (1,)), ((), ())), preferred_element_type=jnp.float32))
        for h in range(2):
            cols = slice(h * LANES, (h + 1) * LANES)
            u_store(0, b, h, jnp.where(row16 < half, out[0][:, cols], out[1][:, cols]))

    def transpose_block(b):
        for m in range(ROWS):
            for h in range(2):
                xt[pl.ds(b * BLOCK + m * TILE, TILE), h * LANES:(h + 1) * LANES] = xv[pl.ds(b * BLOCK + (h * ROWS + m) * LANES, LANES), :].T

    def section_products(par, s):
        first, last = SECTIONS[s]
        if last - first > 1:
            chains = [(b, range(MATMUL_ROWS)) for b in range(first, last)]
        else:
            chains = [(first, range(p * MATMUL_ROWS // 2, (p + 1) * MATMUL_ROWS // 2)) for p in range(2)]
        groups = [(b, h) for b in range(first, last) for h in range(2)]
        spare = ROWS - MATMUL_ROWS
        accs = {}

        def vector_step(b, h, f, i):
            t = xt[pl.ds(b * BLOCK + (MATMUL_ROWS + i) * TILE + f, ROWS), h * LANES:(h + 1) * LANES].astype(jnp.float32) * dcol[f:f + ROWS, :]
            t = t[:SUB] + t[SUB:]
            accs[b, h, i] = accs[b, h, i] + t if f else t

        pending = [(b, h, f, i) for b, h in groups for f in range(0, TILE, ROWS) for i in range(spare)]
        steps = len(chains[0][1])
        outs = [None] * len(chains)
        for k in range(steps):
            for c, (b, ms) in enumerate(chains):
                m = ms[k]
                u = jnp.dot(dmat[:, m * TILE:(m + 1) * TILE], xt[pl.ds(b * BLOCK + m * TILE, TILE), :], preferred_element_type=jnp.float32)
                outs[c] = u if k == 0 else outs[c] + u
            for args in pending[len(pending) * k // steps:len(pending) * (k + 1) // steps]:
                vector_step(*args)
            if k + 1 < steps and (k + 1) % FENCE == 0:
                pl.delay(1)
        for b, h in groups:
            cols = slice(h * LANES, (h + 1) * LANES)
            if last - first > 1:
                u = outs[b - first][:, cols]
            else:
                u = jnp.where(row16 < MATMUL_ROWS // 2, outs[0][:, cols], outs[1][:, cols])
            high = u[SUB:]
            for i in range(spare):
                high = jnp.where(row8 == MATMUL_ROWS + i - SUB, jnp.sum(accs[b, h, i], axis=0, keepdims=True), high)
            u_store(par, b, h, jnp.concatenate([u[:SUB], high], axis=0))

    def products(par):
        for s in range(len(SECTIONS)):
            section_products(par, s)
            u_send(par, s)

    def r_copy(buf, s):
        here = buf.at[rows_of(s)]
        return pltpu.make_async_remote_copy(src_ref=here, dst_ref=here, send_sem=rsend_sem.at[s], recv_sem=rrecv_sem.at[s], device_id={'feat': sibling}, device_id_type=MESH)

    def new_residual(par, s, factor):
        rows = rows_of(s)
        for d in range(1, size):
            src = lax.rem(me + d, size)
            there = ubuf.at[par, src, rows]
            pltpu.make_async_remote_copy(src_ref=there, dst_ref=there, send_sem=send_sem.at[par, s, 0], recv_sem=recv_sem.at[par, s, src], device_id={'feat': src}, device_id_type=MESH).wait_recv()
        total = ubuf[par, 0, rows, :].astype(jnp.float32)
        for k in range(1, size):
            total = total + ubuf[par, k, rows, :].astype(jnp.float32)
        return res[rows, :] - factor * total

    def gradient(par, factor):
        for s in range(len(SECTIONS)):
            first, last = SECTIONS[s]
            rows = rows_of(s)

            @pl.when(lead)
            def _():
                r = new_residual(par, s, factor)
                res[rows, :] = r
                rbf[rows, :] = r.astype(jnp.bfloat16)
                r_copy(rbf, s).start()

            @pl.when(core == 0)
            def _():
                r_copy(rbf, s).wait_recv()

            pieces = (last - first) * ROWS
            sums = [None] * 2
            for j in range(pieces // 2):
                for q in range(2):
                    k = first * QROWS + q * pieces + 2 * j
                    r16 = rbf[pl.ds(k // ROWS * ROWS, ROWS), :].astype(jnp.float32)
                    left = jnp.concatenate([jnp.where(row16 == (k + e) % ROWS, r16, 0.0).astype(jnp.bfloat16) for e in range(2)], axis=1)
                    g = jnp.dot(left, xv[pl.ds(k * LANES, TILE), :], preferred_element_type=jnp.float32)
                    sums[q] = g if j == 0 else sums[q] + g
            for q in range(2):
                if s:
                    sums[q] = gref[q] + sums[q]
                if s < len(SECTIONS) - 1:
                    gref[q] = sums[q]
        sums = [jnp.sum(g, axis=0, keepdims=True) for g in sums]
        return (sums[0] + sums[1]) * (1.0 / samples)

    def update(grad):
        weights = wcur[...]
        eta = eta_v[...]
        threshold = eta * lasso_weight
        stepped = weights + eta * grad
        shrunk = jnp.maximum(stepped - threshold, 0.0) + jnp.minimum(stepped + threshold, 0.0)
        change = shrunk - weights
        wcur[...] = weights + COMBINE_WEIGHT * change
        set_left(change, MATMUL_ROWS)
        set_column(change)

    small[0].wait()
    set_left(wcur[...], ROWS)
    for s, (first, last) in enumerate(SECTIONS):
        for b in range(first, last):
            loads[b].wait()
            first_products(b)
            transpose_block(b)
        if s == 0:
            pl.semaphore_wait(barrier, size - 1)
        u_send(0, s)
    small[1].wait()
    small[2].wait()

    @pl.loop(0, SWEEPS)
    def _(t):
        par = lax.rem(t, 2)
        factor = jnp.where(t == 0, 1.0, COMBINE_WEIGHT).astype(jnp.float32)
        update(gradient(par, factor))
        products(1 - par)
        u_wait_sends(par)

        @pl.when(lead)
        def _():
            for s in range(len(SECTIONS)):
                r_copy(rbf, s).wait_send()

    par = SWEEPS % 2
    w_out[...] = wcur[...]
    for s in range(len(SECTIONS)):
        @pl.when(lead)
        def _():
            res[rows_of(s), :] = new_residual(par, s, COMBINE_WEIGHT)
            r_copy(res, s).start()
    for s in range(len(SECTIONS)):
        @pl.when(core == 0)
        def _():
            r_copy(res, s).wait_recv()
    r_out[...] = res[...]
    u_wait_sends(par)

    @pl.when(lead)
    def _():
        for s in range(len(SECTIONS)):
            r_copy(res, s).wait_send()


def solution(mesh):
    size = mesh.shape['feat']

    def local_run(x_local, coef_local, targets_local, step_local):
        samples, feats = x_local.shape
        sections = len(SECTIONS)
        lasso_weight = 0.3 * size / (feats * size) ** 0.5
        vmem = pl.BlockSpec(memory_space=pltpu.VMEM)
        anywhere = pl.BlockSpec(memory_space=pl.ANY)
        weights, residual = pl.pallas_call(
            functools.partial(kernel, size, lasso_weight),
            out_shape=(jax.ShapeDtypeStruct((1, feats), jnp.float32), jax.ShapeDtypeStruct((samples // LANES, LANES), jnp.float32)),
            in_specs=[anywhere] * 4,
            out_specs=(vmem, vmem),
            scratch_shapes=[
                pltpu.VMEM((samples, feats), jnp.bfloat16),
                pltpu.VMEM((samples, feats), jnp.bfloat16),
                pltpu.VMEM((2, size, samples // LANES, LANES), jnp.bfloat16),
                pltpu.VMEM((samples // LANES, LANES), jnp.bfloat16),
                pltpu.VMEM((samples // LANES, LANES), jnp.float32),
                pltpu.VMEM((ROWS, ROWS * feats), jnp.bfloat16),
                pltpu.VMEM((feats, LANES), jnp.float32),
                pltpu.VMEM((2, ROWS, feats), jnp.float32),
                pltpu.VMEM((1, feats), jnp.float32),
                pltpu.VMEM((1, feats), jnp.float32),
                pltpu.SemaphoreType.DMA((samples // BLOCK,)),
                pltpu.SemaphoreType.DMA((3,)),
                pltpu.SemaphoreType.DMA((2, sections, size // 2)),
                pltpu.SemaphoreType.DMA((2, sections, size)),
                pltpu.SemaphoreType.DMA((sections,)),
                pltpu.SemaphoreType.DMA((sections,)),
            ],
            compiler_params=pltpu.CompilerParams(collective_id=0, has_side_effects=True),
        )(x_local, coef_local.reshape(1, feats), targets_local.reshape(samples // LANES, LANES), step_local.reshape(1, feats))
        return weights.reshape(feats, 1), residual.reshape(samples, 1)

    return jax.shard_map(local_run, mesh=mesh, in_specs=(P('prob', 'feat'), P(('prob', 'feat'), None), P('prob', None), P(('prob', 'feat'))), out_specs=(P(('prob', 'feat'), None), P('prob', None)), check_vma=False)
```

```python
import functools

import jax
import jax.numpy as jnp
from jax import lax
from jax.experimental import pallas as pl
from jax.experimental.pallas import tpu as pltpu
from jax.sharding import PartitionSpec as P

SWEEPS = 6
COMBINE_WEIGHT = 0.8
MESH = pl.DeviceIdType.MESH
LANES = 128
SUB = 8
ROWS = 16
TILE = 2 * LANES
BLOCK = ROWS * TILE
QROWS = BLOCK // LANES
MATMUL_ROWS = 10
FENCE = 4
SECTIONS = ((0, 2), (2, 4))


def kernel(size, lasso_weight, x_hbm, w_hbm, y_hbm, eta_hbm, w_out, r_out, xv, xt, ubuf, rbf, res, dmat, dcol, gref, wcur, eta_v, load_sem, small_sem, send_sem, recv_sem, rsend_sem, rrecv_sem):
    samples = x_hbm.shape[0]
    blocks = samples // BLOCK
    chips = size // 2
    me = lax.axis_index('feat')
    chip, core = me // 2, lax.rem(me, 2)
    sibling = 2 * chip + 1 - core
    lead = core == 1
    far_order = [chips // 2] + [d for d in range(1, chips) if d != chips // 2]

    small = [pltpu.make_async_copy(src, dst, small_sem.at[i]) for i, (src, dst) in enumerate(((w_hbm, wcur), (eta_hbm, eta_v), (y_hbm, res)))]
    loads = [pltpu.make_async_copy(x_hbm.at[pl.ds(b * BLOCK, BLOCK)], xv.at[pl.ds(b * BLOCK, BLOCK)], load_sem.at[b]) for b in range(blocks)]
    small[0].start()
    for load in loads:
        load.start()
    for load in small[1:]:
        load.start()

    barrier = pltpu.get_barrier_semaphore()
    for d in range(1, size):
        pl.semaphore_signal(barrier, inc=1, device_id={'feat': lax.rem(me + d, size)}, device_id_type=MESH)

    row16 = lax.broadcasted_iota(jnp.int32, (ROWS, LANES), 0)
    row8 = lax.broadcasted_iota(jnp.int32, (SUB, LANES), 0)

    def set_left(values, rows):
        for h in range(2):
            spread = jnp.broadcast_to(values[:, h * LANES:(h + 1) * LANES], (ROWS, LANES))
            for m in range(rows):
                dmat[:, m * TILE + h * LANES:m * TILE + (h + 1) * LANES] = jnp.where(row16 == m, spread, 0.0).astype(jnp.bfloat16)

    def set_column(values):
        rounded = values.astype(jnp.bfloat16).astype(jnp.float32)
        for h in range(2):
            dcol[h * LANES:(h + 1) * LANES, :] = jnp.broadcast_to(rounded[:, h * LANES:(h + 1) * LANES], (LANES, LANES)).T

    def rows_of(s):
        first, last = SECTIONS[s]
        return pl.ds(first * QROWS, (last - first) * QROWS)

    def u_copy(par, s, dest, slot):
        here = ubuf.at[par, me, rows_of(s)]
        return pltpu.make_async_remote_copy(src_ref=here, dst_ref=here, send_sem=send_sem.at[par, s, slot], recv_sem=recv_sem.at[par, s, me], device_id={'feat': dest}, device_id_type=MESH)

    def u_send(par, s):
        for slot, d in enumerate(far_order):
            u_copy(par, s, 2 * lax.rem(chip + d, chips) + 1, slot).start()

        @pl.when(core == 0)
        def _():
            u_copy(par, s, sibling, chips - 1).start()

    def u_wait_sends(par):
        for s in range(len(SECTIONS)):
            for slot in range(chips - 1):
                u_copy(par, s, sibling, slot).wait_send()

            @pl.when(core == 0)
            def _():
                u_copy(par, s, sibling, chips - 1).wait_send()

    def u_store(par, b, h, values):
        ubuf[par, me, pl.ds(b * QROWS + h * ROWS, ROWS), :] = values.astype(jnp.bfloat16)

    def first_products(b):
        rhs = []
        for m in range(ROWS):
            rhs.append(jnp.concatenate([xv[pl.ds(b * BLOCK + (h * ROWS + m) * LANES, LANES), :] for h in range(2)], axis=0))
        half = ROWS // 2
        out = []
        for p in range(2):
            left = dmat[:, p * half * TILE:(p + 1) * half * TILE]
            right = jnp.concatenate(rhs[p * half:(p + 1) * half], axis=1)
            out.append(lax.dot_general(left, right, (((1,), (1,)), ((), ())), preferred_element_type=jnp.float32))
        for h in range(2):
            cols = slice(h * LANES, (h + 1) * LANES)
            u_store(0, b, h, jnp.where(row16 < half, out[0][:, cols], out[1][:, cols]))

    def transpose_block(b):
        for m in range(ROWS):
            for h in range(2):
                xt[pl.ds(b * BLOCK + m * TILE, TILE), h * LANES:(h + 1) * LANES] = xv[pl.ds(b * BLOCK + (h * ROWS + m) * LANES, LANES), :].T

    def section_products(par, s):
        first, last = SECTIONS[s]
        if last - first > 1:
            chains = [(b, range(MATMUL_ROWS)) for b in range(first, last)]
        else:
            chains = [(first, range(p * MATMUL_ROWS // 2, (p + 1) * MATMUL_ROWS // 2)) for p in range(2)]
        groups = [(b, h) for b in range(first, last) for h in range(2)]
        spare = ROWS - MATMUL_ROWS
        accs = {}

        def vector_step(b, h, f, i):
            t = xt[pl.ds(b * BLOCK + (MATMUL_ROWS + i) * TILE + f, ROWS), h * LANES:(h + 1) * LANES].astype(jnp.float32) * dcol[f:f + ROWS, :]
            t = t[:SUB] + t[SUB:]
            accs[b, h, i] = accs[b, h, i] + t if f else t

        pending = [(b, h, f, i) for b, h in groups for f in range(0, TILE, ROWS) for i in range(spare)]
        steps = len(chains[0][1])
        outs = [None] * len(chains)
        for k in range(steps):
            for c, (b, ms) in enumerate(chains):
                m = ms[k]
                u = jnp.dot(dmat[:, m * TILE:(m + 1) * TILE], xt[pl.ds(b * BLOCK + m * TILE, TILE), :], preferred_element_type=jnp.float32)
                outs[c] = u if k == 0 else outs[c] + u
            for args in pending[len(pending) * k // steps:len(pending) * (k + 1) // steps]:
                vector_step(*args)
            if k + 1 < steps and (k + 1) % FENCE == 0:
                pl.delay(1)
        for b, h in groups:
            cols = slice(h * LANES, (h + 1) * LANES)
            if last - first > 1:
                u = outs[b - first][:, cols]
            else:
                u = jnp.where(row16 < MATMUL_ROWS // 2, outs[0][:, cols], outs[1][:, cols])
            high = u[SUB:]
            for i in range(spare):
                high = jnp.where(row8 == MATMUL_ROWS + i - SUB, jnp.sum(accs[b, h, i], axis=0, keepdims=True), high)
            u_store(par, b, h, jnp.concatenate([u[:SUB], high], axis=0))

    def products(par):
        for s in range(len(SECTIONS)):
            section_products(par, s)
            u_send(par, s)

    def r_copy(buf, s):
        here = buf.at[rows_of(s)]
        return pltpu.make_async_remote_copy(src_ref=here, dst_ref=here, send_sem=rsend_sem.at[s], recv_sem=rrecv_sem.at[s], device_id={'feat': sibling}, device_id_type=MESH)

    def new_residual(par, s, factor):
        rows = rows_of(s)
        for d in range(1, size):
            src = lax.rem(me + d, size)
            there = ubuf.at[par, src, rows]
            pltpu.make_async_remote_copy(src_ref=there, dst_ref=there, send_sem=send_sem.at[par, s, 0], recv_sem=recv_sem.at[par, s, src], device_id={'feat': src}, device_id_type=MESH).wait_recv()
        total = ubuf[par, 0, rows, :].astype(jnp.float32)
        for k in range(1, size):
            total = total + ubuf[par, k, rows, :].astype(jnp.float32)
        return res[rows, :] - factor * total

    def gradient(par, factor):
        for s in range(len(SECTIONS)):
            first, last = SECTIONS[s]
            rows = rows_of(s)

            @pl.when(lead)
            def _():
                r = new_residual(par, s, factor)
                res[rows, :] = r
                rbf[rows, :] = r.astype(jnp.bfloat16)
                r_copy(rbf, s).start()

            @pl.when(core == 0)
            def _():
                r_copy(rbf, s).wait_recv()

            pieces = (last - first) * ROWS
            sums = [None] * 2
            for j in range(pieces // 2):
                for q in range(2):
                    k = first * QROWS + q * pieces + 2 * j
                    r16 = rbf[pl.ds(k // ROWS * ROWS, ROWS), :].astype(jnp.float32)
                    left = jnp.concatenate([jnp.where(row16 == (k + e) % ROWS, r16, 0.0).astype(jnp.bfloat16) for e in range(2)], axis=1)
                    g = jnp.dot(left, xv[pl.ds(k * LANES, TILE), :], preferred_element_type=jnp.float32)
                    sums[q] = g if j == 0 else sums[q] + g
            for q in range(2):
                if s:
                    sums[q] = gref[q] + sums[q]
                if s < len(SECTIONS) - 1:
                    gref[q] = sums[q]
        sums = [jnp.sum(g, axis=0, keepdims=True) for g in sums]
        return (sums[0] + sums[1]) * (1.0 / samples)

    def update(grad):
        weights = wcur[...]
        eta = eta_v[...]
        threshold = eta * lasso_weight
        stepped = weights + eta * grad
        shrunk = jnp.maximum(stepped - threshold, 0.0) + jnp.minimum(stepped + threshold, 0.0)
        change = shrunk - weights
        wcur[...] = weights + COMBINE_WEIGHT * change
        set_left(change, MATMUL_ROWS)
        set_column(change)

    small[0].wait()
    set_left(wcur[...], ROWS)
    for s, (first, last) in enumerate(SECTIONS):
        for b in range(first, last):
            loads[b].wait()
            first_products(b)
            transpose_block(b)
        if s == 0:
            pl.semaphore_wait(barrier, size - 1)
        u_send(0, s)
    small[1].wait()
    small[2].wait()

    @pl.loop(0, SWEEPS)
    def _(t):
        par = lax.rem(t, 2)
        factor = jnp.where(t == 0, 1.0, COMBINE_WEIGHT).astype(jnp.float32)
        update(gradient(par, factor))
        products(1 - par)
        u_wait_sends(par)

        @pl.when(lead)
        def _():
            for s in range(len(SECTIONS)):
                r_copy(rbf, s).wait_send()

    par = SWEEPS % 2
    w_out[...] = wcur[...]
    for s in range(len(SECTIONS)):
        @pl.when(lead)
        def _():
            res[rows_of(s), :] = new_residual(par, s, COMBINE_WEIGHT)
            r_copy(res, s).start()
    for s in range(len(SECTIONS)):
        @pl.when(core == 0)
        def _():
            r_copy(res, s).wait_recv()
    r_out[...] = res[...]
    u_wait_sends(par)

    @pl.when(lead)
    def _():
        for s in range(len(SECTIONS)):
            r_copy(res, s).wait_send()


def solution(mesh):
    size = mesh.shape['feat']

    def local_run(x_local, coef_local, targets_local, step_local):
        samples, feats = x_local.shape
        sections = len(SECTIONS)
        lasso_weight = 0.3 * size / (feats * size) ** 0.5
        vmem = pl.BlockSpec(memory_space=pltpu.VMEM)
        anywhere = pl.BlockSpec(memory_space=pl.ANY)
        weights, residual = pl.pallas_call(
            functools.partial(kernel, size, lasso_weight),
            out_shape=(pltpu.VMEM((1, feats), jnp.float32), pltpu.VMEM((samples // LANES, LANES), jnp.float32)),
            in_specs=[anywhere] * 4,
            out_specs=(vmem, vmem),
            scratch_shapes=[
                pltpu.VMEM((samples, feats), jnp.bfloat16),
                pltpu.VMEM((samples, feats), jnp.bfloat16),
                pltpu.VMEM((2, size, samples // LANES, LANES), jnp.bfloat16),
                pltpu.VMEM((samples // LANES, LANES), jnp.bfloat16),
                pltpu.VMEM((samples // LANES, LANES), jnp.float32),
                pltpu.VMEM((ROWS, ROWS * feats), jnp.bfloat16),
                pltpu.VMEM((feats, LANES), jnp.float32),
                pltpu.VMEM((2, ROWS, feats), jnp.float32),
                pltpu.VMEM((1, feats), jnp.float32),
                pltpu.VMEM((1, feats), jnp.float32),
                pltpu.SemaphoreType.DMA((samples // BLOCK,)),
                pltpu.SemaphoreType.DMA((3,)),
                pltpu.SemaphoreType.DMA((2, sections, size // 2)),
                pltpu.SemaphoreType.DMA((2, sections, size)),
                pltpu.SemaphoreType.DMA((sections,)),
                pltpu.SemaphoreType.DMA((sections,)),
            ],
            compiler_params=pltpu.CompilerParams(collective_id=0, has_side_effects=True),
        )(x_local, coef_local.reshape(1, feats), targets_local.reshape(samples // LANES, LANES), step_local.reshape(1, feats))
        return weights.reshape(feats, 1), residual.reshape(samples, 1)

    return jax.shard_map(local_run, mesh=mesh, in_specs=(P('prob', 'feat'), P(('prob', 'feat'), None), P('prob', None), P(('prob', 'feat'))), out_specs=(P(('prob', 'feat'), None), P('prob', None)), check_vma=False)
```

```python
import functools

import jax
import jax.numpy as jnp
from jax import lax
from jax.experimental import pallas as pl
from jax.experimental.pallas import tpu as pltpu
from jax.sharding import PartitionSpec as P

SWEEPS = 6
COMBINE_WEIGHT = 0.8
MESH = pl.DeviceIdType.MESH
LANES = 128
SUB = 8
ROWS = 16
TILE = 2 * LANES
BLOCK = ROWS * TILE
QROWS = BLOCK // LANES
MATMUL_ROWS = (10, 10)
GRADIENT_ROWS = (24, 24)
GRADIENT_PAUSES = ((), ())
HOIST = 512
PAUSES = ((), (5,))
IDLE = (0, 0)
SECTIONS = ((0, 2), (2, 4))


def kernel(size, lasso_weight, x_hbm, w_hbm, y_hbm, eta_hbm, w_out, r_out, xv, xt, ubuf, rbf, res, dmat, dcol, gref, vref, wcur, eta_v, load_sem, small_sem, send_sem, recv_sem, rsend_sem, rrecv_sem):
    samples = x_hbm.shape[0]
    blocks = samples // BLOCK
    chips = size // 2
    me = lax.axis_index('feat')
    chip, core = me // 2, lax.rem(me, 2)
    sibling = 2 * chip + 1 - core
    lead = core == 1
    far_order = [chips // 2] + [d for d in range(1, chips) if d != chips // 2]

    small = [pltpu.make_async_copy(src, dst, small_sem.at[i]) for i, (src, dst) in enumerate(((w_hbm, wcur), (eta_hbm, eta_v), (y_hbm, res)))]
    loads = [pltpu.make_async_copy(x_hbm.at[pl.ds(b * BLOCK, BLOCK)], xv.at[pl.ds(b * BLOCK, BLOCK)], load_sem.at[b]) for b in range(blocks)]
    small[0].start()
    for load in loads:
        load.start()
    for load in small[1:]:
        load.start()

    barrier = pltpu.get_barrier_semaphore()
    for d in range(1, size):
        pl.semaphore_signal(barrier, inc=1, device_id={'feat': lax.rem(me + d, size)}, device_id_type=MESH)

    row16 = lax.broadcasted_iota(jnp.int32, (ROWS, LANES), 0)
    row8 = lax.broadcasted_iota(jnp.int32, (SUB, LANES), 0)

    def set_left(values, rows):
        for h in range(2):
            spread = jnp.broadcast_to(values[:, h * LANES:(h + 1) * LANES], (ROWS, LANES))
            for m in range(rows):
                dmat[:, m * TILE + h * LANES:m * TILE + (h + 1) * LANES] = jnp.where(row16 == m, spread, 0.0).astype(jnp.bfloat16)

    def set_column(values):
        rounded = values.astype(jnp.bfloat16).astype(jnp.float32)
        for h in range(2):
            dcol[h * LANES:(h + 1) * LANES, :] = jnp.broadcast_to(rounded[:, h * LANES:(h + 1) * LANES], (LANES, LANES)).T

    def rows_of(s):
        first, last = SECTIONS[s]
        return pl.ds(first * QROWS, (last - first) * QROWS)

    def u_copy(par, s, dest, slot):
        here = ubuf.at[par, me, rows_of(s)]
        return pltpu.make_async_remote_copy(src_ref=here, dst_ref=here, send_sem=send_sem.at[par, s, slot], recv_sem=recv_sem.at[par, s], device_id={'feat': dest}, device_id_type=MESH)

    def u_send(par, s):
        for slot, d in enumerate(far_order):
            u_copy(par, s, 2 * lax.rem(chip + d, chips) + 1, slot).start()

        @pl.when(core == 0)
        def _():
            u_copy(par, s, sibling, chips - 1).start()

    def u_wait_sends(par):
        for s in range(len(SECTIONS)):
            for slot in range(chips - 1):
                u_copy(par, s, sibling, slot).wait_send()

            @pl.when(core == 0)
            def _():
                u_copy(par, s, sibling, chips - 1).wait_send()

    def u_store(par, b, h, values):
        ubuf[par, me, pl.ds(b * QROWS + h * ROWS, ROWS), :] = values.astype(jnp.bfloat16)

    def first_products(b):
        rhs = []
        for m in range(ROWS):
            rhs.append(jnp.concatenate([xv[pl.ds(b * BLOCK + (h * ROWS + m) * LANES, LANES), :] for h in range(2)], axis=0))
        half = ROWS // 2
        out = []
        for p in range(2):
            left = dmat[:, p * half * TILE:(p + 1) * half * TILE]
            right = jnp.concatenate(rhs[p * half:(p + 1) * half], axis=1)
            out.append(lax.dot_general(left, right, (((1,), (1,)), ((), ())), preferred_element_type=jnp.float32))
        for h in range(2):
            cols = slice(h * LANES, (h + 1) * LANES)
            u_store(0, b, h, jnp.where(row16 < half, out[0][:, cols], out[1][:, cols]))

    def transpose_block(b):
        for m in range(ROWS):
            for h in range(2):
                xt[pl.ds(b * BLOCK + m * TILE, TILE), h * LANES:(h + 1) * LANES] = xv[pl.ds(b * BLOCK + (h * ROWS + m) * LANES, LANES), :].T

    def section_products(par, s):
        first, last = SECTIONS[s]
        rows = MATMUL_ROWS[s]
        if last - first > 1:
            chains = [(b, range(rows)) for b in range(first, last)]
        else:
            chains = [(first, range(p * rows // 2, (p + 1) * rows // 2)) for p in range(2)]
        groups = [(b, h) for b in range(first, last) for h in range(2)]
        spare = ROWS - rows
        accs = {}

        def vector_step(b, h, f, i):
            t = xt[pl.ds(b * BLOCK + (rows + i) * TILE + f, ROWS), h * LANES:(h + 1) * LANES].astype(jnp.float32) * dcol[f:f + ROWS, :]
            t = t[:SUB] + t[SUB:]
            accs[b, h, i] = accs[b, h, i] + t if f else t

        pending = [(b, h, f, i) for b, h in groups for f in range(0, TILE, ROWS) for i in range(spare)]
        steps = len(chains[0][1])
        outs = [None] * len(chains)
        for k in range(steps):
            for c, (b, ms) in enumerate(chains):
                m = ms[k]
                u = jnp.dot(dmat[:, m * TILE:(m + 1) * TILE], xt[pl.ds(b * BLOCK + m * TILE, TILE), :], preferred_element_type=jnp.float32)
                outs[c] = u if k == 0 else outs[c] + u
            share = steps - IDLE[s]
            done = max(k - IDLE[s], 0)
            for args in pending[len(pending) * done // share:len(pending) * max(k + 1 - IDLE[s], 0) // share]:
                vector_step(*args)
            if k + 1 in PAUSES[s]:
                pl.delay(1)
        for b, h in groups:
            cols = slice(h * LANES, (h + 1) * LANES)
            if last - first > 1:
                u = outs[b - first][:, cols]
            else:
                u = jnp.where(row16 < rows // 2, outs[0][:, cols], outs[1][:, cols])
            high = u[SUB:]
            for i in range(spare):
                high = jnp.where(row8 == rows + i - SUB, jnp.sum(accs[b, h, i], axis=0, keepdims=True), high)
            u_store(par, b, h, jnp.concatenate([u[:SUB], high], axis=0))

    def products(par):
        for s in range(len(SECTIONS)):
            section_products(par, s)
            u_send(par, s)

    def r_copy(buf, s):
        here = buf.at[rows_of(s)]
        return pltpu.make_async_remote_copy(src_ref=here, dst_ref=here, send_sem=rsend_sem.at[s], recv_sem=rrecv_sem.at[s], device_id={'feat': sibling}, device_id_type=MESH)

    def new_residual(par, s, factor):
        rows = rows_of(s)
        arrived = ubuf.at[par, pl.ds(0, size - 1), rows]
        pltpu.make_async_copy(arrived, arrived, recv_sem.at[par, s]).wait()
        total = ubuf[par, 0, rows, :].astype(jnp.float32)
        for k in range(1, size):
            total = total + ubuf[par, k, rows, :].astype(jnp.float32)
        return res[rows, :] - factor * total

    def gradient(par, factor):
        for s in range(len(SECTIONS)):
            first, last = SECTIONS[s]
            rows = rows_of(s)

            @pl.when(lead)
            def _():
                r = new_residual(par, s, factor)
                res[rows, :] = r
                rbf[rows, :] = r.astype(jnp.bfloat16)
                r_copy(rbf, s).start()

            @pl.when(core == 0)
            def _():
                r_copy(rbf, s).wait_recv()

            groups = list(range(first * QROWS, last * QROWS))
            spare = groups[len(groups) - GRADIENT_ROWS[s]:] if GRADIENT_ROWS[s] else []
            groups = groups[:len(groups) - len(spare)]
            sums = [None] * 2
            extra = [None] * 2
            columns = {}

            def vector_step(k, f):
                if f == 0:
                    columns[k] = jnp.broadcast_to(rbf[k // ROWS * ROWS:(k // ROWS + 1) * ROWS, :].astype(jnp.float32)[k % ROWS:k % ROWS + 1], (LANES, LANES)).T
                t = xv[pl.ds(k * LANES + f, ROWS), :].astype(jnp.float32)
                for h in range(2):
                    p = t[:, h * LANES:(h + 1) * LANES] * columns[k][f:f + ROWS]
                    p = p[:SUB] + p[SUB:]
                    extra[h] = p if extra[h] is None else extra[h] + p

            pending = [(k, f) for k in spare for f in range(0, LANES, ROWS)]
            steps = len(groups) // 4
            half = len(groups) // 2
            for j in range(steps):
                for q in range(2):
                    k = groups[q * half + 2 * j]
                    r16 = rbf[pl.ds(k // ROWS * ROWS, ROWS), :].astype(jnp.float32)
                    left = jnp.concatenate([jnp.where(row16 == (k + e) % ROWS, r16, 0.0).astype(jnp.bfloat16) for e in range(2)], axis=1)
                    g = jnp.dot(left, xv[pl.ds(k * LANES, TILE), :], preferred_element_type=jnp.float32)
                    sums[q] = g if j == 0 else sums[q] + g
                for args in pending[len(pending) * j // steps:len(pending) * (j + 1) // steps]:
                    vector_step(*args)
                if j + 1 in GRADIENT_PAUSES[s]:
                    pl.delay(1)
            if spare:
                vsum = jnp.concatenate(extra, axis=1)
                if s:
                    vsum = vref[...] + vsum
                if s < len(SECTIONS) - 1:
                    vref[...] = vsum
            elif s:
                vsum = vref[...]
            else:
                vref[...] = jnp.zeros_like(vref)
            for q in range(2):
                if s:
                    sums[q] = gref[q] + sums[q]
                if s < len(SECTIONS) - 1:
                    gref[q] = sums[q]
        sums = [jnp.sum(g, axis=0, keepdims=True) for g in sums]
        sums.append(jnp.sum(vsum, axis=0, keepdims=True))
        return (sums[0] + sums[1] + sums[2]) * (1.0 / samples)

    def update(grad):
        weights = wcur[...]
        eta = eta_v[...]
        threshold = eta * lasso_weight
        stepped = weights + eta * grad
        shrunk = jnp.maximum(stepped - threshold, 0.0) + jnp.minimum(stepped + threshold, 0.0)
        change = shrunk - weights
        wcur[...] = weights + COMBINE_WEIGHT * change
        set_left(change, max(MATMUL_ROWS))
        set_column(change)

    small[0].wait()
    set_left(wcur[...], ROWS)
    for s, (first, last) in enumerate(SECTIONS):
        for b in range(first, last):
            loads[b].wait()
            first_products(b)
            transpose_block(b)
        if s == 0:
            pl.semaphore_wait(barrier, size - 1)
        u_send(0, s)
    small[1].wait()
    small[2].wait()

    @pl.loop(0, SWEEPS)
    def _(t):
        par = lax.rem(t, 2)
        factor = jnp.where(t == 0, 1.0, COMBINE_WEIGHT).astype(jnp.float32)
        update(gradient(par, factor))
        products(1 - par)
        u_wait_sends(par)

        @pl.when(lead)
        def _():
            for s in range(len(SECTIONS)):
                r_copy(rbf, s).wait_send()

    par = SWEEPS % 2
    w_out[...] = wcur[...]
    for s in range(len(SECTIONS)):
        @pl.when(lead)
        def _():
            res[rows_of(s), :] = new_residual(par, s, COMBINE_WEIGHT)
            r_copy(res, s).start()
    for s in range(len(SECTIONS)):
        @pl.when(core == 0)
        def _():
            r_copy(res, s).wait_recv()
    r_out[...] = res[...]
    u_wait_sends(par)

    @pl.when(lead)
    def _():
        for s in range(len(SECTIONS)):
            r_copy(res, s).wait_send()


def solution(mesh):
    size = mesh.shape['feat']

    def local_run(x_local, coef_local, targets_local, step_local):
        samples, feats = x_local.shape
        sections = len(SECTIONS)
        lasso_weight = 0.3 * size / (feats * size) ** 0.5
        vmem = pl.BlockSpec(memory_space=pltpu.VMEM)
        anywhere = pl.BlockSpec(memory_space=pl.ANY)
        weights, residual = pl.pallas_call(
            functools.partial(kernel, size, lasso_weight),
            out_shape=(pltpu.VMEM((1, feats), jnp.float32), pltpu.VMEM((samples // LANES, LANES), jnp.float32)),
            in_specs=[anywhere] * 4,
            out_specs=(vmem, vmem),
            scratch_shapes=[
                pltpu.VMEM((samples, feats), jnp.bfloat16),
                pltpu.VMEM((samples, feats), jnp.bfloat16),
                pltpu.VMEM((2, size, samples // LANES, LANES), jnp.bfloat16),
                pltpu.VMEM((samples // LANES, LANES), jnp.bfloat16),
                pltpu.VMEM((samples // LANES, LANES), jnp.float32),
                pltpu.VMEM((ROWS, ROWS * feats), jnp.bfloat16),
                pltpu.VMEM((feats, LANES), jnp.float32),
                pltpu.VMEM((2, ROWS, feats), jnp.float32),
                pltpu.VMEM((SUB, feats), jnp.float32),
                pltpu.VMEM((1, feats), jnp.float32),
                pltpu.VMEM((1, feats), jnp.float32),
                pltpu.SemaphoreType.DMA((samples // BLOCK,)),
                pltpu.SemaphoreType.DMA((3,)),
                pltpu.SemaphoreType.DMA((2, sections, size // 2)),
                pltpu.SemaphoreType.DMA((2, sections)),
                pltpu.SemaphoreType.DMA((sections,)),
                pltpu.SemaphoreType.DMA((sections,)),
            ],
            compiler_params=pltpu.CompilerParams(collective_id=0, has_side_effects=True),
        )(x_local, coef_local.reshape(1, feats), targets_local.reshape(samples // LANES, LANES), step_local.reshape(1, feats))
        return weights.reshape(feats, 1), residual.reshape(samples, 1)

    return jax.shard_map(local_run, mesh=mesh, in_specs=(P('prob', 'feat'), P(('prob', 'feat'), None), P('prob', None), P(('prob', 'feat'))), out_specs=(P(('prob', 'feat'), None), P('prob', None)), check_vma=False)
```

```python
import functools

import jax
import jax.numpy as jnp
from jax import lax
from jax.experimental import pallas as pl
from jax.experimental.pallas import tpu as pltpu
from jax.sharding import PartitionSpec as P

SWEEPS = 6
COMBINE_WEIGHT = 0.8
MESH = pl.DeviceIdType.MESH
LANES = 128
SUB = 8
ROWS = 16
TILE = 2 * LANES
BLOCK = ROWS * TILE
QROWS = BLOCK // LANES
MATMUL_ROWS = (10, 10)
FIRST_ROWS = 8
GRADIENT_ROWS = (24, 24)
GRADIENT_PAUSES = ((), ())
HOIST = 512
PAUSES = ((), (5,))
IDLE = (0, 0)
SECTIONS = ((0, 2), (2, 4))


def kernel(size, lasso_weight, x_hbm, w_hbm, y_hbm, eta_hbm, w_out, r_out, xv, xt, ubuf, rbf, res, dmat, dcol, gref, vref, wcur, eta_v, load_sem, small_sem, send_sem, recv_sem, rsend_sem, rrecv_sem):
    samples = x_hbm.shape[0]
    blocks = samples // BLOCK
    chips = size // 2
    me = lax.axis_index('feat')
    chip, core = me // 2, lax.rem(me, 2)
    sibling = 2 * chip + 1 - core
    lead = core == 1
    far_order = [chips // 2] + [d for d in range(1, chips) if d != chips // 2]
    far_leads = [2 * lax.rem(chip + d, chips) + 1 for d in far_order]

    small = [pltpu.make_async_copy(src, dst, small_sem.at[i]) for i, (src, dst) in enumerate(((w_hbm, wcur), (eta_hbm, eta_v), (y_hbm, res)))]
    loads = [pltpu.make_async_copy(x_hbm.at[pl.ds(b * BLOCK, BLOCK)], xv.at[pl.ds(b * BLOCK, BLOCK)], load_sem.at[b]) for b in range(blocks)]
    small[0].start()
    for load in loads:
        load.start()
    for load in small[1:]:
        load.start()

    barrier = pltpu.get_barrier_semaphore()
    for d in range(1, size):
        pl.semaphore_signal(barrier, inc=1, device_id={'feat': lax.rem(me + d, size)}, device_id_type=MESH)

    row16 = lax.broadcasted_iota(jnp.int32, (ROWS, LANES), 0)
    row8 = lax.broadcasted_iota(jnp.int32, (SUB, LANES), 0)

    def set_left(values, rows):
        for h in range(2):
            spread = jnp.broadcast_to(values[:, h * LANES:(h + 1) * LANES], (ROWS, LANES))
            for m in range(rows):
                dmat[:, m * TILE + h * LANES:m * TILE + (h + 1) * LANES] = jnp.where(row16 == m, spread, 0.0).astype(jnp.bfloat16)

    def set_column(values):
        rounded = values.astype(jnp.bfloat16).astype(jnp.float32)
        for h in range(2):
            dcol[h * LANES:(h + 1) * LANES, :] = jnp.broadcast_to(rounded[:, h * LANES:(h + 1) * LANES], (LANES, LANES)).T

    def rows_of(s):
        first, last = SECTIONS[s]
        return pl.ds(first * QROWS, (last - first) * QROWS)

    def u_copy(par, s, dest, slot):
        here = ubuf.at[par, me, rows_of(s)]
        return pltpu.make_async_remote_copy(src_ref=here, dst_ref=here, send_sem=send_sem.at[par, s, slot], recv_sem=recv_sem.at[par, s], device_id={'feat': dest}, device_id_type=MESH)

    def u_send(par, s):
        for slot, dest in enumerate(far_leads):
            u_copy(par, s, dest, slot).start()

        @pl.when(core == 0)
        def _():
            u_copy(par, s, sibling, chips - 1).start()

    def u_wait_sends(par):
        for s in range(len(SECTIONS)):
            for slot in range(chips - 1):
                u_copy(par, s, sibling, slot).wait_send()

            @pl.when(core == 0)
            def _():
                u_copy(par, s, sibling, chips - 1).wait_send()

    def u_store(par, b, h, values):
        ubuf[par, me, pl.ds(b * QROWS + h * ROWS, ROWS), :] = values.astype(jnp.bfloat16)

    def transpose_tile(b, m):
        for h in range(2):
            xt[pl.ds(b * BLOCK + m * TILE, TILE), h * LANES:(h + 1) * LANES] = xv[pl.ds(b * BLOCK + (h * ROWS + m) * LANES, LANES), :].T

    def first_products(b):
        for m in range(FIRST_ROWS, ROWS):
            transpose_tile(b, m)
        half = FIRST_ROWS // 2
        u = [None] * 2
        for p in range(2):
            ms = range(p * half, (p + 1) * half)
            tiles = [jnp.concatenate([xv[pl.ds(b * BLOCK + (h * ROWS + m) * LANES, LANES), :] for h in range(2)], axis=0) for m in ms]
            u[p] = lax.dot_general(dmat[:, p * half * TILE:(p + 1) * half * TILE], jnp.concatenate(tiles, axis=1), (((1,), (1,)), ((), ())), preferred_element_type=jnp.float32)
        bounds = [0, half, FIRST_ROWS]
        if FIRST_ROWS < ROWS:
            rest = (ROWS - FIRST_ROWS) // 2
            for p in range(2):
                low = FIRST_ROWS + p * rest
                u.append(jnp.dot(dmat[:, low * TILE:(low + rest) * TILE], xt[pl.ds(b * BLOCK + low * TILE, rest * TILE), :], preferred_element_type=jnp.float32))
                bounds.append(low + rest)
        for h in range(2):
            cols = slice(h * LANES, (h + 1) * LANES)
            out = u[-1][:, cols]
            for p in reversed(range(len(u) - 1)):
                out = jnp.where(row16 < bounds[p + 1], u[p][:, cols], out)
            u_store(0, b, h, out)

    def section_products(par, s):
        first, last = SECTIONS[s]
        rows = MATMUL_ROWS[s]
        if last - first > 1:
            chains = [(b, range(rows)) for b in range(first, last)]
        else:
            chains = [(first, range(p * rows // 2, (p + 1) * rows // 2)) for p in range(2)]
        groups = [(b, h) for b in range(first, last) for h in range(2)]
        spare = ROWS - rows
        accs = {}

        def vector_step(b, h, f, i):
            t = xt[pl.ds(b * BLOCK + (rows + i) * TILE + f, ROWS), h * LANES:(h + 1) * LANES].astype(jnp.float32) * dcol[f:f + ROWS, :]
            t = t[:SUB] + t[SUB:]
            accs[b, h, i] = accs[b, h, i] + t if f else t

        pending = [(b, h, f, i) for b, h in groups for f in range(0, TILE, ROWS) for i in range(spare)]
        steps = len(chains[0][1])
        outs = [None] * len(chains)
        for k in range(steps):
            for c, (b, ms) in enumerate(chains):
                m = ms[k]
                u = jnp.dot(dmat[:, m * TILE:(m + 1) * TILE], xt[pl.ds(b * BLOCK + m * TILE, TILE), :], preferred_element_type=jnp.float32)
                outs[c] = u if k == 0 else outs[c] + u
            share = steps - IDLE[s]
            done = max(k - IDLE[s], 0)
            for args in pending[len(pending) * done // share:len(pending) * max(k + 1 - IDLE[s], 0) // share]:
                vector_step(*args)
            if k + 1 in PAUSES[s]:
                pl.delay(1)
        for b, h in groups:
            cols = slice(h * LANES, (h + 1) * LANES)
            if last - first > 1:
                u = outs[b - first][:, cols]
            else:
                u = jnp.where(row16 < rows // 2, outs[0][:, cols], outs[1][:, cols])
            high = u[SUB:]
            for i in range(spare):
                high = jnp.where(row8 == rows + i - SUB, jnp.sum(accs[b, h, i], axis=0, keepdims=True), high)
            u_store(par, b, h, jnp.concatenate([u[:SUB], high], axis=0))

    def products(par):
        for s in range(len(SECTIONS)):
            section_products(par, s)
            u_send(par, s)

    def r_copy(buf, s):
        here = buf.at[rows_of(s)]
        return pltpu.make_async_remote_copy(src_ref=here, dst_ref=here, send_sem=rsend_sem.at[s], recv_sem=rrecv_sem.at[s], device_id={'feat': sibling}, device_id_type=MESH)

    def new_residual(par, s, factor):
        rows = rows_of(s)
        arrived = ubuf.at[par, pl.ds(0, size - 1), rows]
        pltpu.make_async_copy(arrived, arrived, recv_sem.at[par, s]).wait()
        total = ubuf[par, 0, rows, :].astype(jnp.float32)
        for k in range(1, size):
            total = total + ubuf[par, k, rows, :].astype(jnp.float32)
        return res[rows, :] - factor * total

    def gradient(par, factor):
        for s in range(len(SECTIONS)):
            first, last = SECTIONS[s]
            rows = rows_of(s)

            @pl.when(lead)
            def _():
                r = new_residual(par, s, factor)
                res[rows, :] = r
                rbf[rows, :] = r.astype(jnp.bfloat16)
                r_copy(rbf, s).start()

            @pl.when(core == 0)
            def _():
                r_copy(rbf, s).wait_recv()

            groups = list(range(first * QROWS, last * QROWS))
            spare = groups[len(groups) - GRADIENT_ROWS[s]:] if GRADIENT_ROWS[s] else []
            groups = groups[:len(groups) - len(spare)]
            sums = [None] * 2
            extra = [None] * 2
            columns = {}

            def vector_step(k, f):
                if f == 0:
                    columns[k] = jnp.broadcast_to(rbf[k // ROWS * ROWS:(k // ROWS + 1) * ROWS, :].astype(jnp.float32)[k % ROWS:k % ROWS + 1], (LANES, LANES)).T
                t = xv[pl.ds(k * LANES + f, ROWS), :].astype(jnp.float32)
                for h in range(2):
                    p = t[:, h * LANES:(h + 1) * LANES] * columns[k][f:f + ROWS]
                    p = p[:SUB] + p[SUB:]
                    extra[h] = p if extra[h] is None else extra[h] + p

            pending = [(k, f) for k in spare for f in range(0, LANES, ROWS)]
            steps = len(groups) // 4
            half = len(groups) // 2
            for j in range(steps):
                for q in range(2):
                    k = groups[q * half + 2 * j]
                    r16 = rbf[pl.ds(k // ROWS * ROWS, ROWS), :].astype(jnp.float32)
                    left = jnp.concatenate([jnp.where(row16 == (k + e) % ROWS, r16, 0.0).astype(jnp.bfloat16) for e in range(2)], axis=1)
                    g = jnp.dot(left, xv[pl.ds(k * LANES, TILE), :], preferred_element_type=jnp.float32)
                    sums[q] = g if j == 0 else sums[q] + g
                for args in pending[len(pending) * j // steps:len(pending) * (j + 1) // steps]:
                    vector_step(*args)
                if j + 1 in GRADIENT_PAUSES[s]:
                    pl.delay(1)
            if spare:
                vsum = jnp.concatenate(extra, axis=1)
                if s:
                    vsum = vref[...] + vsum
                if s < len(SECTIONS) - 1:
                    vref[...] = vsum
            elif s:
                vsum = vref[...]
            else:
                vref[...] = jnp.zeros_like(vref)
            for q in range(2):
                if s:
                    sums[q] = gref[q] + sums[q]
                if s < len(SECTIONS) - 1:
                    gref[q] = sums[q]
        sums = [jnp.sum(g, axis=0, keepdims=True) for g in sums]
        sums.append(jnp.sum(vsum, axis=0, keepdims=True))
        return (sums[0] + sums[1] + sums[2]) * (1.0 / samples)

    def update(grad):
        weights = wcur[...]
        eta = eta_v[...]
        threshold = eta * lasso_weight
        stepped = weights + eta * grad
        shrunk = jnp.maximum(stepped - threshold, 0.0) + jnp.minimum(stepped + threshold, 0.0)
        change = shrunk - weights
        wcur[...] = weights + COMBINE_WEIGHT * change
        set_left(change, max(MATMUL_ROWS))
        set_column(change)

    small[0].wait()
    set_left(wcur[...], ROWS)
    for s, (first, last) in enumerate(SECTIONS):
        for b in range(first, last):
            loads[b].wait()
            first_products(b)
        if s == 0:
            pl.semaphore_wait(barrier, size - 1)
        u_send(0, s)
    @pl.loop(0, blocks)
    def _(b):
        for m in range(FIRST_ROWS):
            for h in range(2):
                src = pl.multiple_of(b * BLOCK + (h * ROWS + m) * LANES, LANES)
                dst = pl.multiple_of(b * BLOCK + m * TILE, TILE)
                xt[pl.ds(dst, TILE), h * LANES:(h + 1) * LANES] = xv[pl.ds(src, LANES), :].T

    small[1].wait()
    small[2].wait()

    @pl.loop(0, SWEEPS)
    def _(t):
        par = lax.rem(t, 2)
        factor = jnp.where(t == 0, 1.0, COMBINE_WEIGHT).astype(jnp.float32)
        update(gradient(par, factor))
        products(1 - par)
        u_wait_sends(par)

        @pl.when(lead)
        def _():
            for s in range(len(SECTIONS)):
                r_copy(rbf, s).wait_send()

    par = SWEEPS % 2
    w_out[...] = wcur[...]
    for s in range(len(SECTIONS)):
        @pl.when(lead)
        def _():
            res[rows_of(s), :] = new_residual(par, s, COMBINE_WEIGHT)
            r_copy(res, s).start()
    for s in range(len(SECTIONS)):
        @pl.when(core == 0)
        def _():
            r_copy(res, s).wait_recv()
    r_out[...] = res[...]
    u_wait_sends(par)

    @pl.when(lead)
    def _():
        for s in range(len(SECTIONS)):
            r_copy(res, s).wait_send()


def solution(mesh):
    size = mesh.shape['feat']

    def local_run(x_local, coef_local, targets_local, step_local):
        samples, feats = x_local.shape
        sections = len(SECTIONS)
        lasso_weight = 0.3 * size / (feats * size) ** 0.5
        vmem = pl.BlockSpec(memory_space=pltpu.VMEM)
        anywhere = pl.BlockSpec(memory_space=pl.ANY)
        weights, residual = pl.pallas_call(
            functools.partial(kernel, size, lasso_weight),
            out_shape=(pltpu.VMEM((1, feats), jnp.float32), pltpu.VMEM((samples // LANES, LANES), jnp.float32)),
            in_specs=[anywhere] * 4,
            out_specs=(vmem, vmem),
            scratch_shapes=[
                pltpu.VMEM((samples, feats), jnp.bfloat16),
                pltpu.VMEM((samples, feats), jnp.bfloat16),
                pltpu.VMEM((2, size, samples // LANES, LANES), jnp.bfloat16),
                pltpu.VMEM((samples // LANES, LANES), jnp.bfloat16),
                pltpu.VMEM((samples // LANES, LANES), jnp.float32),
                pltpu.VMEM((ROWS, ROWS * feats), jnp.bfloat16),
                pltpu.VMEM((feats, LANES), jnp.float32),
                pltpu.VMEM((2, ROWS, feats), jnp.float32),
                pltpu.VMEM((SUB, feats), jnp.float32),
                pltpu.VMEM((1, feats), jnp.float32),
                pltpu.VMEM((1, feats), jnp.float32),
                pltpu.SemaphoreType.DMA((samples // BLOCK,)),
                pltpu.SemaphoreType.DMA((3,)),
                pltpu.SemaphoreType.DMA((2, sections, size // 2)),
                pltpu.SemaphoreType.DMA((2, sections)),
                pltpu.SemaphoreType.DMA((sections,)),
                pltpu.SemaphoreType.DMA((sections,)),
            ],
            compiler_params=pltpu.CompilerParams(collective_id=0, has_side_effects=True),
        )(x_local, coef_local.reshape(1, feats), targets_local.reshape(samples // LANES, LANES), step_local.reshape(1, feats))
        return weights.reshape(feats, 1), residual.reshape(samples, 1)

    return jax.shard_map(local_run, mesh=mesh, in_specs=(P('prob', 'feat'), P(('prob', 'feat'), None), P('prob', None), P(('prob', 'feat'))), out_specs=(P(('prob', 'feat'), None), P('prob', None)), check_vma=False)
```

```python
import functools

import jax
import jax.numpy as jnp
from jax import lax
from jax.experimental import pallas as pl
from jax.experimental.pallas import tpu as pltpu
from jax.sharding import PartitionSpec as P

SWEEPS = 6
COMBINE_WEIGHT = 0.8
MESH = pl.DeviceIdType.MESH
LANES = 128
SUB = 8
ROWS = 16
TILE = 2 * LANES
BLOCK = ROWS * TILE
QROWS = BLOCK // LANES
MATMUL_ROWS = (10, 10)
FIRST_ROWS = 8
GRADIENT_ROWS = (24, 24)
GRADIENT_PAUSES = ((), ())
HOIST = 512
PAUSES = ((), (5,))
IDLE = (0, 0)
SECTIONS = ((0, 2), (2, 4))


def kernel(size, lasso_weight, x_hbm, w_hbm, y_hbm, eta_hbm, w_out, r_out, xv, xt, ubuf, rbf, res, dmat, dcol, gref, vref, wcur, eta_v, load_sem, small_sem, send_sem, recv_sem, rsend_sem, rrecv_sem):
    samples = x_hbm.shape[0]
    blocks = samples // BLOCK
    chips = size // 2
    me = lax.axis_index('feat')
    chip, core = me // 2, lax.rem(me, 2)
    sibling = 2 * chip + 1 - core
    lead = core == 1
    far_order = [chips // 2] + [d for d in range(1, chips) if d != chips // 2]
    far_leads = [2 * lax.rem(chip + d, chips) + 1 for d in far_order]

    small = [pltpu.make_async_copy(src, dst, small_sem.at[i]) for i, (src, dst) in enumerate(((w_hbm, wcur), (eta_hbm, eta_v), (y_hbm, res)))]
    loads = [pltpu.make_async_copy(x_hbm.at[pl.ds(b * BLOCK, BLOCK)], xv.at[pl.ds(b * BLOCK, BLOCK)], load_sem.at[b]) for b in range(blocks)]
    small[0].start()
    for load in loads:
        load.start()
    for load in small[1:]:
        load.start()

    barrier = pltpu.get_barrier_semaphore()
    for d in range(1, size):
        pl.semaphore_signal(barrier, inc=1, device_id={'feat': lax.rem(me + d, size)}, device_id_type=MESH)

    row16 = lax.broadcasted_iota(jnp.int32, (ROWS, LANES), 0)
    row8 = lax.broadcasted_iota(jnp.int32, (SUB, LANES), 0)

    def set_left(values, rows):
        for h in range(2):
            spread = jnp.broadcast_to(values[:, h * LANES:(h + 1) * LANES], (ROWS, LANES))
            for m in range(rows):
                dmat[:, m * TILE + h * LANES:m * TILE + (h + 1) * LANES] = jnp.where(row16 == m, spread, 0.0).astype(jnp.bfloat16)

    def set_column(values):
        rounded = values.astype(jnp.bfloat16).astype(jnp.float32)
        for h in range(2):
            dcol[h * LANES:(h + 1) * LANES, :] = jnp.broadcast_to(rounded[:, h * LANES:(h + 1) * LANES], (LANES, LANES)).T

    def rows_of(s):
        first, last = SECTIONS[s]
        return pl.ds(first * QROWS, (last - first) * QROWS)

    def u_copy(par, s, dest, slot):
        here = ubuf.at[par, me, rows_of(s)]
        return pltpu.make_async_remote_copy(src_ref=here, dst_ref=here, send_sem=send_sem.at[par, s, slot], recv_sem=recv_sem.at[par, s], device_id={'feat': dest}, device_id_type=MESH)

    def u_send(par, s):
        for slot, dest in enumerate(far_leads):
            u_copy(par, s, dest, slot).start()

        @pl.when(core == 0)
        def _():
            u_copy(par, s, sibling, chips - 1).start()

    def u_wait_sends(par):
        for s in range(len(SECTIONS)):
            for slot in range(chips - 1):
                u_copy(par, s, sibling, slot).wait_send()

            @pl.when(core == 0)
            def _():
                u_copy(par, s, sibling, chips - 1).wait_send()

    def u_store(par, b, h, values):
        ubuf[par, me, pl.ds(b * QROWS + h * ROWS, ROWS), :] = values.astype(jnp.bfloat16)

    def transpose_tile(b, m):
        for h in range(2):
            xt[pl.ds(b * BLOCK + m * TILE, TILE), h * LANES:(h + 1) * LANES] = xv[pl.ds(b * BLOCK + (h * ROWS + m) * LANES, LANES), :].T

    def first_products(b):
        for m in range(FIRST_ROWS, ROWS):
            transpose_tile(b, m)
        half = FIRST_ROWS // 2
        u = [None] * 2
        for p in range(2):
            ms = range(p * half, (p + 1) * half)
            tiles = [jnp.concatenate([xv[pl.ds(b * BLOCK + (h * ROWS + m) * LANES, LANES), :] for h in range(2)], axis=0) for m in ms]
            u[p] = lax.dot_general(dmat[:, p * half * TILE:(p + 1) * half * TILE], jnp.concatenate(tiles, axis=1), (((1,), (1,)), ((), ())), preferred_element_type=jnp.float32)
        bounds = [0, half, FIRST_ROWS]
        if FIRST_ROWS < ROWS:
            rest = (ROWS - FIRST_ROWS) // 2
            for p in range(2):
                low = FIRST_ROWS + p * rest
                u.append(jnp.dot(dmat[:, low * TILE:(low + rest) * TILE], xt[pl.ds(b * BLOCK + low * TILE, rest * TILE), :], preferred_element_type=jnp.float32))
                bounds.append(low + rest)
        for h in range(2):
            cols = slice(h * LANES, (h + 1) * LANES)
            out = u[-1][:, cols]
            for p in reversed(range(len(u) - 1)):
                out = jnp.where(row16 < bounds[p + 1], u[p][:, cols], out)
            u_store(0, b, h, out)

    def section_products(par, s):
        first, last = SECTIONS[s]
        rows = MATMUL_ROWS[s]
        if last - first > 1:
            chains = [(b, range(rows)) for b in range(first, last)]
        else:
            chains = [(first, range(p * rows // 2, (p + 1) * rows // 2)) for p in range(2)]
        groups = [(b, h) for b in range(first, last) for h in range(2)]
        spare = ROWS - rows
        accs = {}

        def vector_step(b, h, f, i):
            t = xt[pl.ds(b * BLOCK + (rows + i) * TILE + f, ROWS), h * LANES:(h + 1) * LANES].astype(jnp.float32) * dcol[f:f + ROWS, :]
            t = t[:SUB] + t[SUB:]
            accs[b, h, i] = accs[b, h, i] + t if f else t

        pending = [(b, h, f, i) for b, h in groups for f in range(0, TILE, ROWS) for i in range(spare)]
        steps = len(chains[0][1])
        outs = [None] * len(chains)
        for k in range(steps):
            for c, (b, ms) in enumerate(chains):
                m = ms[k]
                u = jnp.dot(dmat[:, m * TILE:(m + 1) * TILE], xt[pl.ds(b * BLOCK + m * TILE, TILE), :], preferred_element_type=jnp.float32)
                outs[c] = u if k == 0 else outs[c] + u
            share = steps - IDLE[s]
            done = max(k - IDLE[s], 0)
            for args in pending[len(pending) * done // share:len(pending) * max(k + 1 - IDLE[s], 0) // share]:
                vector_step(*args)
            if k + 1 in PAUSES[s]:
                pl.delay(1)
        for b, h in groups:
            cols = slice(h * LANES, (h + 1) * LANES)
            if last - first > 1:
                u = outs[b - first][:, cols]
            else:
                u = jnp.where(row16 < rows // 2, outs[0][:, cols], outs[1][:, cols])
            high = u[SUB:]
            for i in range(spare):
                high = jnp.where(row8 == rows + i - SUB, jnp.sum(accs[b, h, i], axis=0, keepdims=True), high)
            u_store(par, b, h, jnp.concatenate([u[:SUB], high], axis=0))

    def products(par):
        for s in range(len(SECTIONS)):
            section_products(par, s)
            u_send(par, s)

    def r_copy(buf, s):
        here = buf.at[rows_of(s)]
        return pltpu.make_async_remote_copy(src_ref=here, dst_ref=here, send_sem=rsend_sem.at[s], recv_sem=rrecv_sem.at[s], device_id={'feat': sibling}, device_id_type=MESH)

    def new_residual(par, s, factor):
        rows = rows_of(s)
        arrived = ubuf.at[par, pl.ds(0, size - 1), rows]
        pltpu.make_async_copy(arrived, arrived, recv_sem.at[par, s]).wait()
        total = ubuf[par, 0, rows, :].astype(jnp.float32)
        for k in range(1, size):
            total = total + ubuf[par, k, rows, :].astype(jnp.float32)
        return res[rows, :] - factor * total

    def gradient(par, factor):
        for s in range(len(SECTIONS)):
            first, last = SECTIONS[s]
            rows = rows_of(s)

            @pl.when(lead)
            def _():
                r = new_residual(par, s, factor)
                res[rows, :] = r
                rbf[rows, :] = r.astype(jnp.bfloat16)
                r_copy(rbf, s).start()

            @pl.when(core == 0)
            def _():
                r_copy(rbf, s).wait_recv()

            groups = list(range(first * QROWS, last * QROWS))
            spare = groups[len(groups) - GRADIENT_ROWS[s]:] if GRADIENT_ROWS[s] else []
            groups = groups[:len(groups) - len(spare)]
            sums = [None] * 2
            extra = [None] * 2
            columns = {}

            def vector_step(k, f):
                if f == 0:
                    columns[k] = jnp.broadcast_to(rbf[k // ROWS * ROWS:(k // ROWS + 1) * ROWS, :].astype(jnp.float32)[k % ROWS:k % ROWS + 1], (LANES, LANES)).T
                t = xv[pl.ds(k * LANES + f, ROWS), :].astype(jnp.float32)
                for h in range(2):
                    p = t[:, h * LANES:(h + 1) * LANES] * columns[k][f:f + ROWS]
                    p = p[:SUB] + p[SUB:]
                    extra[h] = p if extra[h] is None else extra[h] + p

            pending = [(k, f) for k in spare for f in range(0, LANES, ROWS)]
            steps = len(groups) // 4
            half = len(groups) // 2
            for j in range(steps):
                for q in range(2):
                    k = groups[q * half + 2 * j]
                    r16 = rbf[pl.ds(k // ROWS * ROWS, ROWS), :].astype(jnp.float32)
                    left = jnp.concatenate([jnp.where(row16 == (k + e) % ROWS, r16, 0.0).astype(jnp.bfloat16) for e in range(2)], axis=1)
                    g = jnp.dot(left, xv[pl.ds(k * LANES, TILE), :], preferred_element_type=jnp.float32)
                    sums[q] = g if j == 0 else sums[q] + g
                for args in pending[len(pending) * j // steps:len(pending) * (j + 1) // steps]:
                    vector_step(*args)
                if j + 1 in GRADIENT_PAUSES[s]:
                    pl.delay(1)
            if spare:
                vsum = jnp.concatenate(extra, axis=1)
                if s:
                    vsum = vref[...] + vsum
                if s < len(SECTIONS) - 1:
                    vref[...] = vsum
            elif s:
                vsum = vref[...]
            else:
                vref[...] = jnp.zeros_like(vref)
            for q in range(2):
                if s:
                    sums[q] = gref[q] + sums[q]
                if s < len(SECTIONS) - 1:
                    gref[q] = sums[q]
        sums = [jnp.sum(g, axis=0, keepdims=True) for g in sums]
        sums.append(jnp.sum(vsum, axis=0, keepdims=True))
        return (sums[0] + sums[1] + sums[2]) * (1.0 / samples)

    def update(grad):
        weights = wcur[...]
        eta = eta_v[...]
        threshold = eta * lasso_weight
        stepped = weights + eta * grad
        shrunk = jnp.maximum(stepped - threshold, 0.0) + jnp.minimum(stepped + threshold, 0.0)
        change = shrunk - weights
        wcur[...] = weights + COMBINE_WEIGHT * change
        set_left(change, max(MATMUL_ROWS))
        set_column(change)

    small[0].wait()
    set_left(wcur[...], ROWS)
    for s, (first, last) in enumerate(SECTIONS):
        for b in range(first, last):
            loads[b].wait()
            first_products(b)
        if s == 0:
            pl.semaphore_wait(barrier, size - 1)
        u_send(0, s)
    @pl.loop(0, blocks)
    def _(b):
        for m in range(FIRST_ROWS):
            for h in range(2):
                src = pl.multiple_of(b * BLOCK + (h * ROWS + m) * LANES, LANES)
                dst = pl.multiple_of(b * BLOCK + m * TILE, TILE)
                xt[pl.ds(dst, TILE), h * LANES:(h + 1) * LANES] = xv[pl.ds(src, LANES), :].T

    small[1].wait()
    small[2].wait()

    @pl.loop(0, SWEEPS)
    def _(t):
        par = lax.rem(t, 2)
        factor = jnp.where(t == 0, 1.0, COMBINE_WEIGHT).astype(jnp.float32)
        update(gradient(par, factor))
        products(1 - par)
        u_wait_sends(par)

        @pl.when(lead)
        def _():
            for s in range(len(SECTIONS)):
                r_copy(rbf, s).wait_send()

    par = SWEEPS % 2
    w_out[...] = wcur[...]
    for s in range(len(SECTIONS)):
        @pl.when(lead)
        def _():
            res[rows_of(s), :] = new_residual(par, s, COMBINE_WEIGHT)
            r_copy(res, s).start()
    for s in range(len(SECTIONS)):
        @pl.when(core == 0)
        def _():
            r_copy(res, s).wait_recv()
    r_out[...] = res[...]
    u_wait_sends(par)

    @pl.when(lead)
    def _():
        for s in range(len(SECTIONS)):
            r_copy(res, s).wait_send()


def put(w_ref, r_ref, w_hbm, r_hbm, sem):
    copies = [pltpu.make_async_copy(src, dst, sem.at[i]) for i, (src, dst) in enumerate(((r_ref, r_hbm), (w_ref, w_hbm)))]
    for copy in copies:
        copy.start()
    for copy in copies:
        copy.wait()


def solution(mesh):
    size = mesh.shape['feat']

    def local_run(x_local, coef_local, targets_local, step_local):
        samples, feats = x_local.shape
        sections = len(SECTIONS)
        lasso_weight = 0.3 * size / (feats * size) ** 0.5
        vmem = pl.BlockSpec(memory_space=pltpu.VMEM)
        anywhere = pl.BlockSpec(memory_space=pl.ANY)
        weights, residual = pl.pallas_call(
            functools.partial(kernel, size, lasso_weight),
            out_shape=(pltpu.VMEM((1, feats), jnp.float32), pltpu.VMEM((samples // LANES, LANES), jnp.float32)),
            in_specs=[anywhere] * 4,
            out_specs=(vmem, vmem),
            scratch_shapes=[
                pltpu.VMEM((samples, feats), jnp.bfloat16),
                pltpu.VMEM((samples, feats), jnp.bfloat16),
                pltpu.VMEM((2, size, samples // LANES, LANES), jnp.bfloat16),
                pltpu.VMEM((samples // LANES, LANES), jnp.bfloat16),
                pltpu.VMEM((samples // LANES, LANES), jnp.float32),
                pltpu.VMEM((ROWS, ROWS * feats), jnp.bfloat16),
                pltpu.VMEM((feats, LANES), jnp.float32),
                pltpu.VMEM((2, ROWS, feats), jnp.float32),
                pltpu.VMEM((SUB, feats), jnp.float32),
                pltpu.VMEM((1, feats), jnp.float32),
                pltpu.VMEM((1, feats), jnp.float32),
                pltpu.SemaphoreType.DMA((samples // BLOCK,)),
                pltpu.SemaphoreType.DMA((3,)),
                pltpu.SemaphoreType.DMA((2, sections, size // 2)),
                pltpu.SemaphoreType.DMA((2, sections)),
                pltpu.SemaphoreType.DMA((sections,)),
                pltpu.SemaphoreType.DMA((sections,)),
            ],
            compiler_params=pltpu.CompilerParams(collective_id=0, has_side_effects=True),
        )(x_local, coef_local.reshape(1, feats), targets_local.reshape(samples // LANES, LANES), step_local.reshape(1, feats))
        weights = pltpu.with_memory_space_constraint(weights, pltpu.VMEM)
        residual = pltpu.with_memory_space_constraint(residual, pltpu.VMEM)
        weights, residual = pl.pallas_call(
            put,
            out_shape=(jax.ShapeDtypeStruct(weights.shape, jnp.float32), jax.ShapeDtypeStruct(residual.shape, jnp.float32)),
            in_specs=[vmem, vmem],
            out_specs=(anywhere, anywhere),
            scratch_shapes=[pltpu.SemaphoreType.DMA((2,))],
        )(weights, residual)
        return weights.reshape(feats, 1), residual.reshape(samples, 1)

    return jax.shard_map(local_run, mesh=mesh, in_specs=(P('prob', 'feat'), P(('prob', 'feat'), None), P('prob', None), P(('prob', 'feat'))), out_specs=(P(('prob', 'feat'), None), P('prob', None)), check_vma=False)
```

```python
import functools

import jax
import jax.numpy as jnp
from jax import lax
from jax.experimental import pallas as pl
from jax.experimental.pallas import tpu as pltpu
from jax.sharding import PartitionSpec as P

SWEEPS = 6
COMBINE_WEIGHT = 0.8
MESH = pl.DeviceIdType.MESH
LANES = 128
SUB = 8
ROWS = 16
TILE = 2 * LANES
BLOCK = ROWS * TILE
QROWS = BLOCK // LANES
MATMUL_ROWS = (10, 10)
FIRST_ROWS = 8
GRADIENT_ROWS = (16, 24)
GRADIENT_PAUSES = ((), ())
HOIST = 512
PAUSES = ((), (5,))
IDLE = (0, 0)
SECTIONS = ((0, 2), (2, 4))


def kernel(size, lasso_weight, x_hbm, w_hbm, y_hbm, eta_hbm, w_out, r_out, xv, xt, ubuf, rbf, res, dmat, dcol, gref, vref, wcur, eta_v, load_sem, small_sem, send_sem, recv_sem, pair_sem, rsend_sem, rrecv_sem):
    samples = x_hbm.shape[0]
    blocks = samples // BLOCK
    chips = size // 2
    me = lax.axis_index('feat')
    chip, core = me // 2, lax.rem(me, 2)
    sibling = 2 * chip + 1 - core
    lead = core == 1
    far_order = [chips // 2] + [d for d in range(1, chips) if d != chips // 2]
    far_leads = [2 * lax.rem(chip + d, chips) + 1 for d in far_order]

    small = [pltpu.make_async_copy(src, dst, small_sem.at[i]) for i, (src, dst) in enumerate(((w_hbm, wcur), (eta_hbm, eta_v), (y_hbm, res)))]
    loads = [pltpu.make_async_copy(x_hbm.at[pl.ds(b * BLOCK, BLOCK)], xv.at[pl.ds(b * BLOCK, BLOCK)], load_sem.at[b]) for b in range(blocks)]
    small[0].start()
    for load in loads:
        load.start()
    for load in small[1:]:
        load.start()

    barrier = pltpu.get_barrier_semaphore()
    for d in range(1, size):
        pl.semaphore_signal(barrier, inc=1, device_id={'feat': lax.rem(me + d, size)}, device_id_type=MESH)

    row16 = lax.broadcasted_iota(jnp.int32, (ROWS, LANES), 0)
    row8 = lax.broadcasted_iota(jnp.int32, (SUB, LANES), 0)

    def set_left(values, rows):
        for h in range(2):
            spread = jnp.broadcast_to(values[:, h * LANES:(h + 1) * LANES], (ROWS, LANES))
            for m in range(rows):
                dmat[:, m * TILE + h * LANES:m * TILE + (h + 1) * LANES] = jnp.where(row16 == m, spread, 0.0).astype(jnp.bfloat16)

    def set_column(values):
        rounded = values.astype(jnp.bfloat16).astype(jnp.float32)
        for h in range(2):
            dcol[h * LANES:(h + 1) * LANES, :] = jnp.broadcast_to(rounded[:, h * LANES:(h + 1) * LANES], (LANES, LANES)).T

    def rows_of(s):
        first, last = SECTIONS[s]
        return pl.ds(first * QROWS, (last - first) * QROWS)

    def u_copy(par, s, dest, slot):
        here = ubuf.at[par, me, rows_of(s)]
        return pltpu.make_async_remote_copy(src_ref=here, dst_ref=here, send_sem=send_sem.at[par, s, slot], recv_sem=recv_sem.at[par, s], device_id={'feat': dest}, device_id_type=MESH)

    def u_send(par, s):
        for slot, dest in enumerate(far_leads):
            u_copy(par, s, dest, slot).start()

    def pair_copy(par):
        here = ubuf.at[par, 2 * chip]
        return pltpu.make_async_remote_copy(src_ref=here, dst_ref=here, send_sem=pair_sem.at[0, par], recv_sem=pair_sem.at[1, par], device_id={'feat': sibling}, device_id_type=MESH)

    def pair_send(par):
        @pl.when(core == 0)
        def _():
            pair_copy(par).start()

    def u_wait_sends(par):
        for s in range(len(SECTIONS)):
            for slot in range(chips - 1):
                u_copy(par, s, sibling, slot).wait_send()

        @pl.when(core == 0)
        def _():
            pair_copy(par).wait_send()

    def u_store(par, b, h, values):
        ubuf[par, me, pl.ds(b * QROWS + h * ROWS, ROWS), :] = values.astype(jnp.bfloat16)

    def transpose_tile(b, m):
        for h in range(2):
            xt[pl.ds(b * BLOCK + m * TILE, TILE), h * LANES:(h + 1) * LANES] = xv[pl.ds(b * BLOCK + (h * ROWS + m) * LANES, LANES), :].T

    def first_products(b):
        for m in range(FIRST_ROWS, ROWS):
            transpose_tile(b, m)
        half = FIRST_ROWS // 2
        u = [None] * 2
        for p in range(2):
            ms = range(p * half, (p + 1) * half)
            tiles = [jnp.concatenate([xv[pl.ds(b * BLOCK + (h * ROWS + m) * LANES, LANES), :] for h in range(2)], axis=0) for m in ms]
            u[p] = lax.dot_general(dmat[:, p * half * TILE:(p + 1) * half * TILE], jnp.concatenate(tiles, axis=1), (((1,), (1,)), ((), ())), preferred_element_type=jnp.float32)
        bounds = [0, half, FIRST_ROWS]
        if FIRST_ROWS < ROWS:
            rest = (ROWS - FIRST_ROWS) // 2
            for p in range(2):
                low = FIRST_ROWS + p * rest
                u.append(jnp.dot(dmat[:, low * TILE:(low + rest) * TILE], xt[pl.ds(b * BLOCK + low * TILE, rest * TILE), :], preferred_element_type=jnp.float32))
                bounds.append(low + rest)
        for h in range(2):
            cols = slice(h * LANES, (h + 1) * LANES)
            out = u[-1][:, cols]
            for p in reversed(range(len(u) - 1)):
                out = jnp.where(row16 < bounds[p + 1], u[p][:, cols], out)
            u_store(0, b, h, out)

    def section_products(par, s):
        first, last = SECTIONS[s]
        rows = MATMUL_ROWS[s]
        if last - first > 1:
            chains = [(b, range(rows)) for b in range(first, last)]
        else:
            chains = [(first, range(p * rows // 2, (p + 1) * rows // 2)) for p in range(2)]
        groups = [(b, h) for b in range(first, last) for h in range(2)]
        spare = ROWS - rows
        accs = {}

        def vector_step(b, h, f, i):
            t = xt[pl.ds(b * BLOCK + (rows + i) * TILE + f, ROWS), h * LANES:(h + 1) * LANES].astype(jnp.float32) * dcol[f:f + ROWS, :]
            t = t[:SUB] + t[SUB:]
            accs[b, h, i] = accs[b, h, i] + t if f else t

        pending = [(b, h, f, i) for b, h in groups for f in range(0, TILE, ROWS) for i in range(spare)]
        steps = len(chains[0][1])
        outs = [None] * len(chains)
        for k in range(steps):
            for c, (b, ms) in enumerate(chains):
                m = ms[k]
                u = jnp.dot(dmat[:, m * TILE:(m + 1) * TILE], xt[pl.ds(b * BLOCK + m * TILE, TILE), :], preferred_element_type=jnp.float32)
                outs[c] = u if k == 0 else outs[c] + u
            share = steps - IDLE[s]
            done = max(k - IDLE[s], 0)
            for args in pending[len(pending) * done // share:len(pending) * max(k + 1 - IDLE[s], 0) // share]:
                vector_step(*args)
            if k + 1 in PAUSES[s]:
                pl.delay(1)
        for b, h in groups:
            cols = slice(h * LANES, (h + 1) * LANES)
            if last - first > 1:
                u = outs[b - first][:, cols]
            else:
                u = jnp.where(row16 < rows // 2, outs[0][:, cols], outs[1][:, cols])
            high = u[SUB:]
            for i in range(spare):
                high = jnp.where(row8 == rows + i - SUB, jnp.sum(accs[b, h, i], axis=0, keepdims=True), high)
            u_store(par, b, h, jnp.concatenate([u[:SUB], high], axis=0))

    def products(par):
        for s in range(len(SECTIONS)):
            section_products(par, s)
            u_send(par, s)
            pl.delay(1)
        pair_send(par)

    def r_copy(buf, s):
        here = buf.at[rows_of(s)]
        return pltpu.make_async_remote_copy(src_ref=here, dst_ref=here, send_sem=rsend_sem.at[s], recv_sem=rrecv_sem.at[s], device_id={'feat': sibling}, device_id_type=MESH)

    def new_residual(par, s, factor):
        rows = rows_of(s)
        arrived = ubuf.at[par, pl.ds(0, size - 2), rows]
        pltpu.make_async_copy(arrived, arrived, recv_sem.at[par, s]).wait()
        if s == 0:
            pair_copy(par).wait_recv()
        total = ubuf[par, 0, rows, :].astype(jnp.float32)
        for k in range(1, size):
            total = total + ubuf[par, k, rows, :].astype(jnp.float32)
        return res[rows, :] - factor * total

    def gradient(par, factor):
        for s in range(len(SECTIONS)):
            first, last = SECTIONS[s]
            rows = rows_of(s)

            @pl.when(lead)
            def _():
                r = new_residual(par, s, factor)
                res[rows, :] = r
                rbf[rows, :] = r.astype(jnp.bfloat16)
                r_copy(rbf, s).start()

            @pl.when(core == 0)
            def _():
                r_copy(rbf, s).wait_recv()

            groups = list(range(first * QROWS, last * QROWS))
            spare = groups[len(groups) - GRADIENT_ROWS[s]:] if GRADIENT_ROWS[s] else []
            groups = groups[:len(groups) - len(spare)]
            sums = [None] * 2
            extra = [None] * 2
            columns = {}

            def vector_step(k, f):
                if f == 0:
                    columns[k] = jnp.broadcast_to(rbf[k // ROWS * ROWS:(k // ROWS + 1) * ROWS, :].astype(jnp.float32)[k % ROWS:k % ROWS + 1], (LANES, LANES)).T
                t = xv[pl.ds(k * LANES + f, ROWS), :].astype(jnp.float32)
                for h in range(2):
                    p = t[:, h * LANES:(h + 1) * LANES] * columns[k][f:f + ROWS]
                    p = p[:SUB] + p[SUB:]
                    extra[h] = p if extra[h] is None else extra[h] + p

            pending = [(k, f) for k in spare for f in range(0, LANES, ROWS)]
            steps = len(groups) // 4
            half = len(groups) // 2
            for j in range(steps):
                for q in range(2):
                    k = groups[q * half + 2 * j]
                    r16 = rbf[pl.ds(k // ROWS * ROWS, ROWS), :].astype(jnp.float32)
                    left = jnp.concatenate([jnp.where(row16 == (k + e) % ROWS, r16, 0.0).astype(jnp.bfloat16) for e in range(2)], axis=1)
                    g = jnp.dot(left, xv[pl.ds(k * LANES, TILE), :], preferred_element_type=jnp.float32)
                    sums[q] = g if j == 0 else sums[q] + g
                for args in pending[len(pending) * j // steps:len(pending) * (j + 1) // steps]:
                    vector_step(*args)
                if j + 1 in GRADIENT_PAUSES[s]:
                    pl.delay(1)
            if spare:
                vsum = jnp.concatenate(extra, axis=1)
                if s:
                    vsum = vref[...] + vsum
                if s < len(SECTIONS) - 1:
                    vref[...] = vsum
            elif s:
                vsum = vref[...]
            else:
                vref[...] = jnp.zeros_like(vref)
            for q in range(2):
                if s:
                    sums[q] = gref[q] + sums[q]
                if s < len(SECTIONS) - 1:
                    gref[q] = sums[q]
        sums = [jnp.sum(g, axis=0, keepdims=True) for g in sums]
        sums.append(jnp.sum(vsum, axis=0, keepdims=True))
        return (sums[0] + sums[1] + sums[2]) * (1.0 / samples)

    def update(grad):
        weights = wcur[...]
        eta = eta_v[...]
        threshold = eta * lasso_weight
        stepped = weights + eta * grad
        shrunk = jnp.maximum(stepped - threshold, 0.0) + jnp.minimum(stepped + threshold, 0.0)
        change = shrunk - weights
        wcur[...] = weights + COMBINE_WEIGHT * change
        set_left(change, max(MATMUL_ROWS))
        set_column(change)

    small[0].wait()
    set_left(wcur[...], ROWS)
    for s, (first, last) in enumerate(SECTIONS):
        for b in range(first, last):
            loads[b].wait()
            first_products(b)
        if s == 0:
            pl.semaphore_wait(barrier, size - 1)
        u_send(0, s)
    pair_send(0)
    @pl.loop(0, blocks)
    def _(b):
        for m in range(FIRST_ROWS):
            for h in range(2):
                src = pl.multiple_of(b * BLOCK + (h * ROWS + m) * LANES, LANES)
                dst = pl.multiple_of(b * BLOCK + m * TILE, TILE)
                xt[pl.ds(dst, TILE), h * LANES:(h + 1) * LANES] = xv[pl.ds(src, LANES), :].T

    small[1].wait()
    small[2].wait()

    @pl.loop(0, SWEEPS)
    def _(t):
        par = lax.rem(t, 2)
        factor = jnp.where(t == 0, 1.0, COMBINE_WEIGHT).astype(jnp.float32)
        update(gradient(par, factor))
        products(1 - par)
        u_wait_sends(par)

        @pl.when(lead)
        def _():
            for s in range(len(SECTIONS)):
                r_copy(rbf, s).wait_send()

    par = SWEEPS % 2
    w_out[...] = wcur[...]
    for s in range(len(SECTIONS)):
        @pl.when(lead)
        def _():
            res[rows_of(s), :] = new_residual(par, s, COMBINE_WEIGHT)
            r_copy(res, s).start()
    for s in range(len(SECTIONS)):
        @pl.when(core == 0)
        def _():
            r_copy(res, s).wait_recv()
    r_out[...] = res[...]
    u_wait_sends(par)

    @pl.when(lead)
    def _():
        for s in range(len(SECTIONS)):
            r_copy(res, s).wait_send()


def put(w_ref, r_ref, w_hbm, r_hbm, sem):
    copies = [pltpu.make_async_copy(src, dst, sem.at[i]) for i, (src, dst) in enumerate(((r_ref, r_hbm), (w_ref, w_hbm)))]
    for copy in copies:
        copy.start()
    for copy in copies:
        copy.wait()


def solution(mesh):
    size = mesh.shape['feat']

    def local_run(x_local, coef_local, targets_local, step_local):
        samples, feats = x_local.shape
        sections = len(SECTIONS)
        lasso_weight = 0.3 * size / (feats * size) ** 0.5
        vmem = pl.BlockSpec(memory_space=pltpu.VMEM)
        anywhere = pl.BlockSpec(memory_space=pl.ANY)
        weights, residual = pl.pallas_call(
            functools.partial(kernel, size, lasso_weight),
            out_shape=(pltpu.VMEM((1, feats), jnp.float32), pltpu.VMEM((samples // LANES, LANES), jnp.float32)),
            in_specs=[anywhere] * 4,
            out_specs=(vmem, vmem),
            scratch_shapes=[
                pltpu.VMEM((samples, feats), jnp.bfloat16),
                pltpu.VMEM((samples, feats), jnp.bfloat16),
                pltpu.VMEM((2, size, samples // LANES, LANES), jnp.bfloat16),
                pltpu.VMEM((samples // LANES, LANES), jnp.bfloat16),
                pltpu.VMEM((samples // LANES, LANES), jnp.float32),
                pltpu.VMEM((ROWS, ROWS * feats), jnp.bfloat16),
                pltpu.VMEM((feats, LANES), jnp.float32),
                pltpu.VMEM((2, ROWS, feats), jnp.float32),
                pltpu.VMEM((SUB, feats), jnp.float32),
                pltpu.VMEM((1, feats), jnp.float32),
                pltpu.VMEM((1, feats), jnp.float32),
                pltpu.SemaphoreType.DMA((samples // BLOCK,)),
                pltpu.SemaphoreType.DMA((3,)),
                pltpu.SemaphoreType.DMA((2, sections, size // 2)),
                pltpu.SemaphoreType.DMA((2, sections)),
                pltpu.SemaphoreType.DMA((2, 2)),
                pltpu.SemaphoreType.DMA((sections,)),
                pltpu.SemaphoreType.DMA((sections,)),
            ],
            compiler_params=pltpu.CompilerParams(collective_id=0, has_side_effects=True),
        )(x_local, coef_local.reshape(1, feats), targets_local.reshape(samples // LANES, LANES), step_local.reshape(1, feats))
        weights = pltpu.with_memory_space_constraint(weights, pltpu.VMEM)
        residual = pltpu.with_memory_space_constraint(residual, pltpu.VMEM)
        weights, residual = pl.pallas_call(
            put,
            out_shape=(jax.ShapeDtypeStruct(weights.shape, jnp.float32), jax.ShapeDtypeStruct(residual.shape, jnp.float32)),
            in_specs=[vmem, vmem],
            out_specs=(anywhere, anywhere),
            scratch_shapes=[pltpu.SemaphoreType.DMA((2,))],
        )(weights, residual)
        return weights.reshape(feats, 1), residual.reshape(samples, 1)

    return jax.shard_map(local_run, mesh=mesh, in_specs=(P('prob', 'feat'), P(('prob', 'feat'), None), P('prob', None), P(('prob', 'feat'))), out_specs=(P(('prob', 'feat'), None), P('prob', None)), check_vma=False)
```

```python
import functools

import jax
import jax.numpy as jnp
from jax import lax
from jax.experimental import pallas as pl
from jax.experimental.pallas import tpu as pltpu
from jax.sharding import PartitionSpec as P

SWEEPS = 6
COMBINE_WEIGHT = 0.8
MESH = pl.DeviceIdType.MESH
LANES = 128
SUB = 8
ROWS = 16
TILE = 2 * LANES
BLOCK = ROWS * TILE
QROWS = BLOCK // LANES
MATMUL_ROWS = (10, 10, 10)
FIRST_ROWS = 8
GRADIENT_ROWS = (16, 12, 12)
GRADIENT_PAUSES = ((), (), ())
HOIST = 512
PAUSES = ((), (3,), (3,))
IDLE = (0, 0, 0)
SECTIONS = ((0, 2), (2, 3), (3, 4))


def kernel(size, lasso_weight, x_hbm, w_hbm, y_hbm, eta_hbm, w_out, r_out, xv, xt, ubuf, rbf, res, dmat, dcol, gref, vref, wcur, eta_v, load_sem, small_sem, send_sem, recv_sem, pair_sem, rsend_sem, rrecv_sem):
    samples = x_hbm.shape[0]
    blocks = samples // BLOCK
    chips = size // 2
    me = lax.axis_index('feat')
    chip, core = me // 2, lax.rem(me, 2)
    sibling = 2 * chip + 1 - core
    lead = core == 1
    far_order = [chips // 2] + [d for d in range(1, chips) if d != chips // 2]
    far_leads = [2 * lax.rem(chip + d, chips) + 1 for d in far_order]

    small = [pltpu.make_async_copy(src, dst, small_sem.at[i]) for i, (src, dst) in enumerate(((w_hbm, wcur), (eta_hbm, eta_v), (y_hbm, res)))]
    loads = [pltpu.make_async_copy(x_hbm.at[pl.ds(b * BLOCK, BLOCK)], xv.at[pl.ds(b * BLOCK, BLOCK)], load_sem.at[b]) for b in range(blocks)]
    small[0].start()
    for load in loads:
        load.start()
    for load in small[1:]:
        load.start()

    barrier = pltpu.get_barrier_semaphore()
    for d in range(1, size):
        pl.semaphore_signal(barrier, inc=1, device_id={'feat': lax.rem(me + d, size)}, device_id_type=MESH)

    row16 = lax.broadcasted_iota(jnp.int32, (ROWS, LANES), 0)
    row8 = lax.broadcasted_iota(jnp.int32, (SUB, LANES), 0)

    def set_left(values, rows):
        for h in range(2):
            spread = jnp.broadcast_to(values[:, h * LANES:(h + 1) * LANES], (ROWS, LANES))
            for m in range(rows):
                dmat[:, m * TILE + h * LANES:m * TILE + (h + 1) * LANES] = jnp.where(row16 == m, spread, 0.0).astype(jnp.bfloat16)

    def set_column(values):
        rounded = values.astype(jnp.bfloat16).astype(jnp.float32)
        for h in range(2):
            dcol[h * LANES:(h + 1) * LANES, :] = jnp.broadcast_to(rounded[:, h * LANES:(h + 1) * LANES], (LANES, LANES)).T

    def rows_of(s):
        first, last = SECTIONS[s]
        return pl.ds(first * QROWS, (last - first) * QROWS)

    def u_copy(par, s, dest, slot):
        here = ubuf.at[par, me, rows_of(s)]
        return pltpu.make_async_remote_copy(src_ref=here, dst_ref=here, send_sem=send_sem.at[par, s, slot], recv_sem=recv_sem.at[par, s], device_id={'feat': dest}, device_id_type=MESH)

    def u_send(par, s):
        for slot, dest in enumerate(far_leads):
            u_copy(par, s, dest, slot).start()

    def pair_copy(par):
        here = ubuf.at[par, 2 * chip]
        return pltpu.make_async_remote_copy(src_ref=here, dst_ref=here, send_sem=pair_sem.at[0, par], recv_sem=pair_sem.at[1, par], device_id={'feat': sibling}, device_id_type=MESH)

    def pair_send(par):
        @pl.when(core == 0)
        def _():
            pair_copy(par).start()

    def u_wait_sends(par):
        for s in range(len(SECTIONS)):
            for slot in range(chips - 1):
                u_copy(par, s, sibling, slot).wait_send()

        @pl.when(core == 0)
        def _():
            pair_copy(par).wait_send()

    def u_store(par, b, h, values):
        ubuf[par, me, pl.ds(b * QROWS + h * ROWS, ROWS), :] = values.astype(jnp.bfloat16)

    def transpose_tile(b, m):
        for h in range(2):
            xt[pl.ds(b * BLOCK + m * TILE, TILE), h * LANES:(h + 1) * LANES] = xv[pl.ds(b * BLOCK + (h * ROWS + m) * LANES, LANES), :].T

    def first_products(b):
        for m in range(FIRST_ROWS, ROWS):
            transpose_tile(b, m)
        half = FIRST_ROWS // 2
        u = [None] * 2
        for p in range(2):
            ms = range(p * half, (p + 1) * half)
            tiles = [jnp.concatenate([xv[pl.ds(b * BLOCK + (h * ROWS + m) * LANES, LANES), :] for h in range(2)], axis=0) for m in ms]
            u[p] = lax.dot_general(dmat[:, p * half * TILE:(p + 1) * half * TILE], jnp.concatenate(tiles, axis=1), (((1,), (1,)), ((), ())), preferred_element_type=jnp.float32)
        bounds = [0, half, FIRST_ROWS]
        if FIRST_ROWS < ROWS:
            rest = (ROWS - FIRST_ROWS) // 2
            for p in range(2):
                low = FIRST_ROWS + p * rest
                u.append(jnp.dot(dmat[:, low * TILE:(low + rest) * TILE], xt[pl.ds(b * BLOCK + low * TILE, rest * TILE), :], preferred_element_type=jnp.float32))
                bounds.append(low + rest)
        for h in range(2):
            cols = slice(h * LANES, (h + 1) * LANES)
            out = u[-1][:, cols]
            for p in reversed(range(len(u) - 1)):
                out = jnp.where(row16 < bounds[p + 1], u[p][:, cols], out)
            u_store(0, b, h, out)

    def section_products(par, s):
        first, last = SECTIONS[s]
        rows = MATMUL_ROWS[s]
        if last - first > 1:
            chains = [(b, range(rows)) for b in range(first, last)]
        else:
            chains = [(first, range(p * rows // 2, (p + 1) * rows // 2)) for p in range(2)]
        groups = [(b, h) for b in range(first, last) for h in range(2)]
        spare = ROWS - rows
        accs = {}

        def vector_step(b, h, f, i):
            t = xt[pl.ds(b * BLOCK + (rows + i) * TILE + f, ROWS), h * LANES:(h + 1) * LANES].astype(jnp.float32) * dcol[f:f + ROWS, :]
            t = t[:SUB] + t[SUB:]
            accs[b, h, i] = accs[b, h, i] + t if f else t

        pending = [(b, h, f, i) for b, h in groups for f in range(0, TILE, ROWS) for i in range(spare)]
        steps = len(chains[0][1])
        outs = [None] * len(chains)
        for k in range(steps):
            for c, (b, ms) in enumerate(chains):
                m = ms[k]
                u = jnp.dot(dmat[:, m * TILE:(m + 1) * TILE], xt[pl.ds(b * BLOCK + m * TILE, TILE), :], preferred_element_type=jnp.float32)
                outs[c] = u if k == 0 else outs[c] + u
            share = steps - IDLE[s]
            done = max(k - IDLE[s], 0)
            for args in pending[len(pending) * done // share:len(pending) * max(k + 1 - IDLE[s], 0) // share]:
                vector_step(*args)
            if k + 1 in PAUSES[s]:
                pl.delay(1)
        for b, h in groups:
            cols = slice(h * LANES, (h + 1) * LANES)
            if last - first > 1:
                u = outs[b - first][:, cols]
            else:
                u = jnp.where(row16 < rows // 2, outs[0][:, cols], outs[1][:, cols])
            high = u[SUB:]
            for i in range(spare):
                high = jnp.where(row8 == rows + i - SUB, jnp.sum(accs[b, h, i], axis=0, keepdims=True), high)
            u_store(par, b, h, jnp.concatenate([u[:SUB], high], axis=0))

    def products(par):
        for s in range(len(SECTIONS)):
            section_products(par, s)
            u_send(par, s)
            pl.delay(1)
        pair_send(par)

    def r_copy(buf, s):
        here = buf.at[rows_of(s)]
        return pltpu.make_async_remote_copy(src_ref=here, dst_ref=here, send_sem=rsend_sem.at[s], recv_sem=rrecv_sem.at[s], device_id={'feat': sibling}, device_id_type=MESH)

    def new_residual(par, s, factor):
        rows = rows_of(s)
        arrived = ubuf.at[par, pl.ds(0, size - 2), rows]
        pltpu.make_async_copy(arrived, arrived, recv_sem.at[par, s]).wait()
        if s == 0:
            pair_copy(par).wait_recv()
        total = ubuf[par, 0, rows, :].astype(jnp.float32)
        for k in range(1, size):
            total = total + ubuf[par, k, rows, :].astype(jnp.float32)
        return res[rows, :] - factor * total

    def gradient(par, factor):
        @pl.when(lead)
        def _():
            for s in range(len(SECTIONS)):
                rows = rows_of(s)
                r = new_residual(par, s, factor)
                res[rows, :] = r
                rbf[rows, :] = r.astype(jnp.bfloat16)
                r_copy(rbf, s).start()

        for s in range(len(SECTIONS)):
            first, last = SECTIONS[s]
            rows = rows_of(s)

            @pl.when(core == 0)
            def _():
                r_copy(rbf, s).wait_recv()

            groups = list(range(first * QROWS, last * QROWS))
            spare = groups[len(groups) - GRADIENT_ROWS[s]:] if GRADIENT_ROWS[s] else []
            groups = groups[:len(groups) - len(spare)]
            sums = [None] * 2
            extra = [None] * 2
            columns = {}

            def vector_step(k, f):
                if f == 0:
                    columns[k] = jnp.broadcast_to(rbf[k // ROWS * ROWS:(k // ROWS + 1) * ROWS, :].astype(jnp.float32)[k % ROWS:k % ROWS + 1], (LANES, LANES)).T
                t = xv[pl.ds(k * LANES + f, ROWS), :].astype(jnp.float32)
                for h in range(2):
                    p = t[:, h * LANES:(h + 1) * LANES] * columns[k][f:f + ROWS]
                    p = p[:SUB] + p[SUB:]
                    extra[h] = p if extra[h] is None else extra[h] + p

            pending = [(k, f) for k in spare for f in range(0, LANES, ROWS)]
            steps = len(groups) // 4
            half = len(groups) // 2
            for j in range(steps):
                for q in range(2):
                    k = groups[q * half + 2 * j]
                    r16 = rbf[pl.ds(k // ROWS * ROWS, ROWS), :].astype(jnp.float32)
                    left = jnp.concatenate([jnp.where(row16 == (k + e) % ROWS, r16, 0.0).astype(jnp.bfloat16) for e in range(2)], axis=1)
                    g = jnp.dot(left, xv[pl.ds(k * LANES, TILE), :], preferred_element_type=jnp.float32)
                    sums[q] = g if j == 0 else sums[q] + g
                for args in pending[len(pending) * j // steps:len(pending) * (j + 1) // steps]:
                    vector_step(*args)
                if j + 1 in GRADIENT_PAUSES[s]:
                    pl.delay(1)
            if spare:
                vsum = jnp.concatenate(extra, axis=1)
                if s:
                    vsum = vref[...] + vsum
                if s < len(SECTIONS) - 1:
                    vref[...] = vsum
            elif s:
                vsum = vref[...]
            else:
                vref[...] = jnp.zeros_like(vref)
            for q in range(2):
                if s:
                    sums[q] = gref[q] + sums[q]
                if s < len(SECTIONS) - 1:
                    gref[q] = sums[q]
        sums = [jnp.sum(g, axis=0, keepdims=True) for g in sums]
        sums.append(jnp.sum(vsum, axis=0, keepdims=True))
        return (sums[0] + sums[1] + sums[2]) * (1.0 / samples)

    def update(grad):
        weights = wcur[...]
        eta = eta_v[...]
        threshold = eta * lasso_weight
        stepped = weights + eta * grad
        shrunk = jnp.maximum(stepped - threshold, 0.0) + jnp.minimum(stepped + threshold, 0.0)
        change = shrunk - weights
        wcur[...] = weights + COMBINE_WEIGHT * change
        set_left(change, max(MATMUL_ROWS))
        set_column(change)

    small[0].wait()
    set_left(wcur[...], ROWS)
    for s, (first, last) in enumerate(SECTIONS):
        for b in range(first, last):
            loads[b].wait()
            first_products(b)
        if s == 0:
            pl.semaphore_wait(barrier, size - 1)
        u_send(0, s)
    pair_send(0)
    @pl.loop(0, blocks)
    def _(b):
        for m in range(FIRST_ROWS):
            for h in range(2):
                src = pl.multiple_of(b * BLOCK + (h * ROWS + m) * LANES, LANES)
                dst = pl.multiple_of(b * BLOCK + m * TILE, TILE)
                xt[pl.ds(dst, TILE), h * LANES:(h + 1) * LANES] = xv[pl.ds(src, LANES), :].T

    small[1].wait()
    small[2].wait()

    @pl.loop(0, SWEEPS)
    def _(t):
        par = lax.rem(t, 2)
        factor = jnp.where(t == 0, 1.0, COMBINE_WEIGHT).astype(jnp.float32)
        update(gradient(par, factor))
        products(1 - par)
        u_wait_sends(par)

        @pl.when(lead)
        def _():
            for s in range(len(SECTIONS)):
                r_copy(rbf, s).wait_send()

    par = SWEEPS % 2
    w_out[...] = wcur[...]
    for s in range(len(SECTIONS)):
        @pl.when(lead)
        def _():
            res[rows_of(s), :] = new_residual(par, s, COMBINE_WEIGHT)
            r_copy(res, s).start()
    for s in range(len(SECTIONS)):
        @pl.when(core == 0)
        def _():
            r_copy(res, s).wait_recv()
    r_out[...] = res[...]
    u_wait_sends(par)

    @pl.when(lead)
    def _():
        for s in range(len(SECTIONS)):
            r_copy(res, s).wait_send()


def put(w_ref, r_ref, w_hbm, r_hbm, sem):
    copies = [pltpu.make_async_copy(src, dst, sem.at[i]) for i, (src, dst) in enumerate(((r_ref, r_hbm), (w_ref, w_hbm)))]
    for copy in copies:
        copy.start()
    for copy in copies:
        copy.wait()


def solution(mesh):
    size = mesh.shape['feat']

    def local_run(x_local, coef_local, targets_local, step_local):
        samples, feats = x_local.shape
        sections = len(SECTIONS)
        lasso_weight = 0.3 * size / (feats * size) ** 0.5
        vmem = pl.BlockSpec(memory_space=pltpu.VMEM)
        anywhere = pl.BlockSpec(memory_space=pl.ANY)
        weights, residual = pl.pallas_call(
            functools.partial(kernel, size, lasso_weight),
            out_shape=(pltpu.VMEM((1, feats), jnp.float32), pltpu.VMEM((samples // LANES, LANES), jnp.float32)),
            in_specs=[anywhere] * 4,
            out_specs=(vmem, vmem),
            scratch_shapes=[
                pltpu.VMEM((samples, feats), jnp.bfloat16),
                pltpu.VMEM((samples, feats), jnp.bfloat16),
                pltpu.VMEM((2, size, samples // LANES, LANES), jnp.bfloat16),
                pltpu.VMEM((samples // LANES, LANES), jnp.bfloat16),
                pltpu.VMEM((samples // LANES, LANES), jnp.float32),
                pltpu.VMEM((ROWS, ROWS * feats), jnp.bfloat16),
                pltpu.VMEM((feats, LANES), jnp.float32),
                pltpu.VMEM((2, ROWS, feats), jnp.float32),
                pltpu.VMEM((SUB, feats), jnp.float32),
                pltpu.VMEM((1, feats), jnp.float32),
                pltpu.VMEM((1, feats), jnp.float32),
                pltpu.SemaphoreType.DMA((samples // BLOCK,)),
                pltpu.SemaphoreType.DMA((3,)),
                pltpu.SemaphoreType.DMA((2, sections, size // 2)),
                pltpu.SemaphoreType.DMA((2, sections)),
                pltpu.SemaphoreType.DMA((2, 2)),
                pltpu.SemaphoreType.DMA((sections,)),
                pltpu.SemaphoreType.DMA((sections,)),
            ],
            compiler_params=pltpu.CompilerParams(collective_id=0, has_side_effects=True),
        )(x_local, coef_local.reshape(1, feats), targets_local.reshape(samples // LANES, LANES), step_local.reshape(1, feats))
        weights = pltpu.with_memory_space_constraint(weights, pltpu.VMEM)
        residual = pltpu.with_memory_space_constraint(residual, pltpu.VMEM)
        weights, residual = pl.pallas_call(
            put,
            out_shape=(jax.ShapeDtypeStruct(weights.shape, jnp.float32), jax.ShapeDtypeStruct(residual.shape, jnp.float32)),
            in_specs=[vmem, vmem],
            out_specs=(anywhere, anywhere),
            scratch_shapes=[pltpu.SemaphoreType.DMA((2,))],
        )(weights, residual)
        return weights.reshape(feats, 1), residual.reshape(samples, 1)

    return jax.shard_map(local_run, mesh=mesh, in_specs=(P('prob', 'feat'), P(('prob', 'feat'), None), P('prob', None), P(('prob', 'feat'))), out_specs=(P(('prob', 'feat'), None), P('prob', None)), check_vma=False)
```
